256 devices in a mesh: gx: 16 (over z, x_lo), gz: 16 (over y, x_hi, core).
Axes of the slice: x: 4 (x_hi: 2, x_lo: 2; x = x_hi * 2 + x_lo), y: 4, z: 8, core: 2. Of those that a mesh axis runs over, the one named last changes fastest.
Arguments:
- velocity: float32 [3, 128, 512, 384], P(None, 'gx', 'gz'), may hold values from -6 to 6
- y_gap: float32 [385], replicated, may hold values from 0.2 to 2
Outputs:
- eddy_visc: float32 [128, 512, 384], P('gx', 'gz')
- lm_field: float32 [128, 512, 384], P('gx', 'gz')
- mm_field: float32 [128, 512, 384], P('gx', 'gz')
- coefficient: float32 [384], replicated
The draws below stay inside these ranges and needn't reach their ends.
All inputs are finite; a program needn't handle non-finite values.
Results may differ from the reference program's by a relative error of at most 0.00002.
Values sent between devices are 32-bit elements; how exact they have to be, the bound alone decides.
No kernel may reach another device: no remote copies, remote signals or barrier semaphores. Data moves between devices by JAX's collectives and lax.ppermute only.
A program may use at most 64 MiB of HBM per device.

```python
import math
import jax
import jax.numpy as jnp
from jax import lax

NY = 384
NX = 128
NZ = 512


def block_levels(key, shape, split, smallest, top_value):
    gain, own = 1.0, jax.random.fold_in(key, 6)
    for dim, shards_of in split:
        draws = jnp.exp(jax.random.uniform(jax.random.fold_in(own, dim), (shards_of,), jnp.float32, smallest / len(split), top_value / len(split)))
        gain = gain * jnp.repeat(draws, shape[dim] // shards_of).reshape([-1 if axis == dim else 1 for axis in range(len(shape))])
    return gain


def scatter_about(stream_key, extent, spread, bound, cuts=(), held_as=jnp.bfloat16):
    entries = spread * jax.random.normal(stream_key, extent, jnp.float32)
    if cuts:
        entries = entries * block_levels(stream_key, extent, cuts, -0.22, 0.18)
    return jnp.clip(entries, -bound, bound).astype(held_as)


def setup_inputs(seed: int = 0) -> dict:
    arg_keys = jax.random.split(jax.random.key(seed), 3)
    velocity = scatter_about(arg_keys[0], (3, NX, NZ, NY), 1.0, 6.0, ((1, 16), (2, 16)), jnp.float32)
    y_gap = jnp.clip(jnp.exp(jax.random.uniform(arg_keys[1], (NY + 1,), jnp.float32, math.log(0.2), math.log(2.0))), 0.2, 2.0)
    return dict(velocity=velocity, y_gap=y_gap)


WEIGHTS = (1.0, 1.0, 1.0, 2.0, 2.0, 2.0)

def wall_slope(values, y_gap):
    padded = jnp.pad(values, [(0, 0)] * (values.ndim - 1) + [(1, 1)])
    return (padded[..., 2:] - padded[..., :-2]) / (y_gap[:-1] + y_gap[1:])

def strain_parts(slope_x, slope_y, slope_z):
    return jnp.stack([slope_x[0], slope_y[1], slope_z[2], 0.5 * (slope_y[0] + slope_x[1]), 0.5 * (slope_z[0] + slope_x[2]), 0.5 * (slope_z[1] + slope_y[2])])

def contract(first_part, second_part):
    summed = first_part[0] * second_part[0]
    for component in range(1, 6):
        summed = summed + WEIGHTS[component] * first_part[component] * second_part[component]
    return summed

def magnitude(strain):
    return jnp.sqrt(2.0 * contract(strain, strain))

def pair_products(speeds):
    return jnp.stack([speeds[0] * speeds[0], speeds[1] * speeds[1], speeds[2] * speeds[2], speeds[0] * speeds[1], speeds[0] * speeds[2], speeds[1] * speeds[2]])

def width_square(y_gap):
    return (0.5 * (y_gap[:-1] + y_gap[1:])) ** (2.0 / 3.0)

def germano(smooth_velocity, smooth_pairs, smooth_stress, test_strain, width_sq):
    leonard = smooth_pairs - pair_products(smooth_velocity)
    model_term = 2.0 * width_sq * (smooth_stress - 4.0 * magnitude(test_strain) * test_strain)
    return (contract(leonard, model_term), contract(model_term, model_term))

def periodic_strain(speeds, y_gap):
    slope_x = (jnp.roll(speeds, -1, 1) - jnp.roll(speeds, 1, 1)) * 0.5
    slope_z = (jnp.roll(speeds, -1, 2) - jnp.roll(speeds, 1, 2)) * 0.5
    slope_y = wall_slope(speeds, y_gap)
    return strain_parts(slope_x, slope_y, slope_z)

def periodic_filter(values):
    along_x = 0.25 * jnp.roll(values, 1, 1) + 0.5 * values + 0.25 * jnp.roll(values, -1, 1)
    return 0.25 * jnp.roll(along_x, 1, 2) + 0.5 * along_x + 0.25 * jnp.roll(along_x, -1, 2)

def reference(velocity, y_gap):
    width_sq = width_square(y_gap)
    strain = periodic_strain(velocity, y_gap)
    strain_size = magnitude(strain)
    smooth_velocity = periodic_filter(velocity)
    smooth_pairs = periodic_filter(pair_products(velocity))
    smooth_stress = periodic_filter(strain_size * strain)
    test_strain = periodic_strain(smooth_velocity, y_gap)
    lm_field, mm_field = germano(smooth_velocity, smooth_pairs, smooth_stress, test_strain, width_sq)
    planes = NX * NZ
    numerator = lax.optimization_barrier(jnp.sum(lm_field, axis=(0, 1)))
    denominator = lax.optimization_barrier(jnp.sum(mm_field, axis=(0, 1)))
    coefficient = numerator / planes / (denominator / planes + 1e-06)
    eddy_visc = coefficient * width_sq * strain_size
    return (eddy_visc, lm_field, mm_field, coefficient)
```

```python
import functools

import jax
import jax.numpy as jnp
from jax import lax
from jax.sharding import Mesh
from jax.sharding import PartitionSpec as P

GX = ("gx_0", "gx_1")
GZ = ("gz_0", "gz_1", "gz_2")


WEIGHTS = (1.0, 1.0, 1.0, 2.0, 2.0, 2.0)


def extended(array, sides, width):
    for axis, dim in sides:
        size, length = (lax.axis_size(axis), array.shape[dim])
        up = [(i, (i + 1) % size) for i in range(size)]
        down = [(j, i) for i, j in up]
        last = lax.slice_in_dim(array, length - width, length, axis=dim)
        leading = lax.slice_in_dim(array, 0, width, axis=dim)
        before = lax.ppermute(last, axis, up)
        after = lax.ppermute(leading, axis, down)
        array = jnp.concatenate([before, array, after], axis=dim)
    return array


def over_group(array, axes):
    members = functools.reduce(lambda count, axis: count * lax.axis_size(axis), axes, 1)
    copies = jnp.broadcast_to(array[None], (members, *array.shape))
    return jnp.sum(lax.all_to_all(copies, axes, 0, 0, tiled=True), axis=0)


def over_axes(array):
    for axes in (("gx_0", "gz_2"), ("gx_1", "gz_0", "gz_1")):
        array = over_group(array, axes)
    return array


def wall_slope(values, y_gap):
    padded = jnp.pad(values, [(0, 0)] * (values.ndim - 1) + [(1, 1)])
    return (padded[..., 2:] - padded[..., :-2]) / (y_gap[:-1] + y_gap[1:])


def strain_parts(slope_x, slope_y, slope_z):
    return jnp.stack(
        [
            slope_x[0],
            slope_y[1],
            slope_z[2],
            0.5 * (slope_y[0] + slope_x[1]),
            0.5 * (slope_z[0] + slope_x[2]),
            0.5 * (slope_z[1] + slope_y[2]),
        ]
    )


def contract(first_part, second_part):
    summed = first_part[0] * second_part[0]
    for component in range(1, 6):
        summed = summed + WEIGHTS[component] * first_part[component] * second_part[component]
    return summed


def magnitude(strain):
    return jnp.sqrt(2.0 * contract(strain, strain))


def pair_products(speeds):
    return jnp.stack(
        [
            speeds[0] * speeds[0],
            speeds[1] * speeds[1],
            speeds[2] * speeds[2],
            speeds[0] * speeds[1],
            speeds[0] * speeds[2],
            speeds[1] * speeds[2],
        ]
    )


def width_square(y_gap):
    return (0.5 * (y_gap[:-1] + y_gap[1:])) ** (2.0 / 3.0)


def germano(smooth_velocity, smooth_pairs, smooth_stress, test_strain, width_sq):
    leonard = smooth_pairs - pair_products(smooth_velocity)
    model_term = 2.0 * width_sq * (smooth_stress - 4.0 * magnitude(test_strain) * test_strain)
    return (contract(leonard, model_term), contract(model_term, model_term))


def rim_strain(padded, y_gap):
    slope_x = (padded[:, 2:, 1:-1] - padded[:, :-2, 1:-1]) * 0.5
    slope_z = (padded[:, 1:-1, 2:] - padded[:, 1:-1, :-2]) * 0.5
    slope_y = wall_slope(padded[:, 1:-1, 1:-1], y_gap)
    return strain_parts(slope_x, slope_y, slope_z)


def rim_filter(values):
    along_x = 0.25 * values[:, :-2] + 0.5 * values[:, 1:-1] + 0.25 * values[:, 2:]
    return 0.25 * along_x[:, :, :-2] + 0.5 * along_x[:, :, 1:-1] + 0.25 * along_x[:, :, 2:]


def per_device(velocity, y_gap):
    width_sq = width_square(y_gap)
    padded = extended(velocity, ((GX, 1), (GZ, 2)), 2)
    strain_wide = rim_strain(padded, y_gap)
    size_wide = magnitude(strain_wide)
    inner = padded[:, 1:-1, 1:-1]
    smooth_pairs = rim_filter(pair_products(inner))
    smooth_stress = rim_filter(size_wide * strain_wide)
    smooth_wide = rim_filter(padded)
    smooth_velocity = smooth_wide[:, 1:-1, 1:-1]
    test_strain = rim_strain(smooth_wide, y_gap)
    strain_size = size_wide[1:-1, 1:-1]
    lm_field, mm_field = germano(
        smooth_velocity, smooth_pairs, smooth_stress, test_strain, width_sq
    )
    planes = velocity.shape[1] * lax.axis_size(GX) * velocity.shape[2] * lax.axis_size(GZ)
    plane_pair = jnp.stack([jnp.sum(lm_field, axis=(0, 1)), jnp.sum(mm_field, axis=(0, 1))])
    total_pair = over_axes(plane_pair)
    coefficient = total_pair[0] / planes / (total_pair[1] / planes + 1e-06)
    eddy_visc = coefficient * width_sq * strain_size
    return (eddy_visc, lm_field, mm_field, coefficient)


def solution(mesh):
    torus = Mesh(mesh.devices.reshape(8, 2, 4, 2, 2), ("gx_0", "gx_1", "gz_0", "gz_1", "gz_2"))
    return jax.shard_map(
        per_device,
        mesh=torus,
        in_specs=(P(None, GX, GZ, None), P()),
        out_specs=(P(GX, GZ, None), P(GX, GZ, None), P(GX, GZ, None), P()),
        check_vma=False,
    )
```

```python
import functools

import jax
import jax.numpy as jnp
from jax import lax
from jax.experimental import pallas as pl
from jax.experimental.pallas import tpu as pltpu
from jax.sharding import Mesh
from jax.sharding import PartitionSpec as P

GX = ("gx_0", "gx_1")
GZ = ("gz_0", "gz_1", "gz_2")

LANES = 128
SUB = 8
TOP = 8
HALO = 2


def neighbours(array, axis, dim, width):
    size, length = (lax.axis_size(axis), array.shape[dim])
    up = [(i, (i + 1) % size) for i in range(size)]
    down = [(j, i) for i, j in up]
    last = lax.slice_in_dim(array, length - width, length, axis=dim)
    leading = lax.slice_in_dim(array, 0, width, axis=dim)
    return lax.ppermute(last, axis, up), lax.ppermute(leading, axis, down)


def over_group(array, axes):
    members = functools.reduce(lambda count, axis: count * lax.axis_size(axis), axes, 1)
    copies = jnp.broadcast_to(array[None], (members, *array.shape))
    return jnp.sum(lax.all_to_all(copies, axes, 0, 0, tiled=True), axis=0)


def over_axes(array):
    for axes in (("gx_0", "gz_2"), ("gx_1", "gz_0", "gz_1")):
        array = over_group(array, axes)
    return array


def width_square(y_gap):
    return (0.5 * (y_gap[:-1] + y_gap[1:])) ** (2.0 / 3.0)


def strain_of(ref, slopes, at, chunk, row):
    def cell(k, step_x=0, step_z=0):
        return ref[k, at + step_x, chunk, pl.ds(row + step_z, SUB), :]

    along_x = [cell(k, 1) - cell(k, -1) for k in range(3)]
    along_z = [cell(k, 0, 1) - cell(k, 0, -1) for k in range(3)]
    parts = [
        along_x[0],
        slopes[1],
        along_z[2],
        slopes[0] + along_x[1],
        along_z[0] + along_x[2],
        along_z[1] + slopes[2],
    ]
    squares = [part * part for part in parts]
    square = 0.5 * (squares[0] + squares[1] + squares[2]) + 0.25 * (
        squares[3] + squares[4] + squares[5]
    )
    return parts, jnp.sqrt(square)


def wall_slopes(read, inverse, chunks):
    lane = lax.broadcasted_iota(jnp.int32, (SUB, LANES), 1)
    values = [read(c) for c in range(chunks)]
    ahead = [pltpu.roll(value, LANES - 1, 1) for value in values] + [jnp.zeros_like(values[0])]
    behind = [jnp.zeros_like(values[0])] + [pltpu.roll(value, 1, 1) for value in values]
    return [
        (
            jnp.where(lane == LANES - 1, ahead[c + 1], ahead[c])
            - jnp.where(lane == 0, behind[c], behind[c + 1])
        )
        * inverse[c]
        for c in range(chunks)
    ]


PAIRS = ((0, 0), (1, 1), (2, 2), (0, 1), (0, 2), (1, 2))


def smooth(below, here, above):
    return (below + above) + (here + here)


def fields_kernel(
    v_ref, before_x, after_x, before_z, after_z, corner_before, corner_after, inv_ref, width_ref,
    lm_ref, mm_ref, size_ref, sums_ref,
    cells, slope, products, filtered, smoothed, smoothed_slope, totals,
):
    nx, nz, ny = v_ref.shape[1:]
    chunks = ny // LANES
    blocks = nz // SUB
    columns = [slice(c * LANES, (c + 1) * LANES) for c in range(chunks)]

    def fill(at, main, low, high):
        for k in range(3):
            for c in range(chunks):
                cells[k, at, c, TOP : TOP + nz, :] = main(k)[:, columns[c]]
                cells[k, at, c, TOP - HALO : TOP, :] = low(k)[:, columns[c]]
                cells[k, at, c, TOP + nz : TOP + nz + HALO, :] = high(k)[:, columns[c]]

    def fill_own(i, carry):
        fill(i + HALO, lambda k: v_ref[k, i], lambda k: before_z[k, i], lambda k: after_z[k, i])
        return carry

    lax.fori_loop(0, nx, fill_own, 0)
    for j in range(HALO):
        fill(j, lambda k: before_x[k, j], lambda k: corner_before[k, j], lambda k: corner_after[k, j])
        m = HALO + j
        fill(nx + m, lambda k: after_x[k, j], lambda k: corner_before[k, m], lambda k: corner_after[k, m])

    inverse = [jnp.broadcast_to(inv_ref[:, columns[c]], (SUB, LANES)) for c in range(chunks)]
    width = [jnp.broadcast_to(width_ref[:, columns[c]], (SUB, LANES)) for c in range(chunks)]

    wide = [TOP - 1 + SUB * b for b in range(blocks + 1)]

    def layer(i, carry):
        at = i + 1
        for row in wide:
            per_speed = [
                wall_slopes(lambda c: cells[k, at, c, pl.ds(row, SUB), :], inverse, chunks)
                for k in range(3)
            ]
            for c in range(chunks):
                parts, size = strain_of(cells, [per_speed[k][c] for k in range(3)], at, c, row)
                slope[c, pl.ds(row, SUB), :] = size
                speeds = [cells[k, at, c, pl.ds(row, SUB), :] for k in range(3)]
                for n in range(6):
                    products[n, c, pl.ds(row, SUB), :] = size * parts[n]
                    p, q = PAIRS[n]
                    products[6 + n, c, pl.ds(row, SUB), :] = speeds[p] * speeds[q]
        for c in range(chunks):
            for b in range(blocks):
                row = TOP + SUB * b
                for n in range(12):
                    filtered[n, i, c, pl.ds(SUB * b, SUB), :] = smooth(
                        products[n, c, pl.ds(row - 1, SUB), :],
                        products[n, c, pl.ds(row, SUB), :],
                        products[n, c, pl.ds(row + 1, SUB), :],
                    )

        @pl.when(jnp.logical_and(i >= 1, i <= nx))
        def _():
            for c in range(chunks):
                for b in range(blocks):
                    size_ref[i - 1, SUB * b : SUB * (b + 1), columns[c]] = slope[
                        c, TOP + SUB * b : TOP + SUB * (b + 1), :
                    ]

        for k in range(3):
            for c in range(chunks):
                for b in range(blocks + 2):
                    row = SUB * b
                    products[k, c, pl.ds(row, SUB), :] = smooth(
                        cells[k, at - 1, c, pl.ds(row, SUB), :],
                        cells[k, at, c, pl.ds(row, SUB), :],
                        cells[k, at + 1, c, pl.ds(row, SUB), :],
                    )
                for row in wide:
                    smoothed[k, i, c, pl.ds(row, SUB), :] = smooth(
                        products[k, c, pl.ds(row - 1, SUB), :],
                        products[k, c, pl.ds(row, SUB), :],
                        products[k, c, pl.ds(row + 1, SUB), :],
                    )
        return carry

    lax.fori_loop(0, nx + 2, layer, 0)

    totals[...] = jnp.zeros_like(totals)

    def result(i, carry):
        at = i + 1
        for b in range(blocks):
            row = TOP + SUB * b
            per_speed = [
                wall_slopes(lambda c: smoothed[k, at, c, pl.ds(row, SUB), :], inverse, chunks)
                for k in range(3)
            ]
            for c in range(chunks):
                parts, size = strain_of(smoothed, [per_speed[k][c] for k in range(3)], at, c, row)
                size = 0.25 * size
                speeds = [0.25 * smoothed[k, at, c, pl.ds(row, SUB), :] for k in range(3)]

                def over_x(n):
                    return smooth(*[filtered[n, i + s, c, pl.ds(SUB * b, SUB), :] for s in range(3)])

                cross, diagonal, outside = [], [], []
                for n in range(6):
                    model = over_x(n) - size * parts[n]
                    p, q = PAIRS[n]
                    cross.append((over_x(6 + n) - speeds[p] * speeds[q]) * model)
                    (diagonal if n < 3 else outside).append(model * model)
                add = functools.partial(functools.reduce, jnp.add)
                lm = (width[c] * (1.0 / 256.0)) * add(cross)
                mm = (width[c] * width[c] * (1.0 / 256.0)) * (add(diagonal) + 0.5 * add(outside))
                lm_ref[i, SUB * b : SUB * (b + 1), columns[c]] = lm
                mm_ref[i, SUB * b : SUB * (b + 1), columns[c]] = mm
                totals[0, c] += lm
                totals[1, c] += mm
        return carry

    lax.fori_loop(0, nx, result, 0)
    for n in range(2):
        for c in range(chunks):
            sums_ref[n : n + 1, columns[c]] = jnp.sum(totals[n, c], axis=0, keepdims=True)


def fields(v, halos, inverse, width_sq):
    _, nx, nz, ny = v.shape
    chunks, rows = ny // LANES, nz + 2 * SUB
    block = jax.ShapeDtypeStruct((nx, nz, ny), jnp.float32)
    scratch = lambda *shape: pltpu.VMEM((*shape, LANES), jnp.float32)
    return pl.pallas_call(
        fields_kernel,
        out_shape=(block, block, block, jax.ShapeDtypeStruct((2, ny), jnp.float32)),
        scratch_shapes=[
            scratch(3, nx + 4, chunks, rows),
            scratch(chunks, rows),
            scratch(12, chunks, rows),
            scratch(12, nx + 2, chunks, nz),
            scratch(3, nx + 2, chunks, rows),
            scratch(1, 1),
            scratch(2, chunks, SUB),
        ],
        name="fields",
        cost_estimate=pl.CostEstimate(flops=40_000_000, bytes_accessed=8_000_000, transcendentals=400_000),
    )(v, *halos, inverse[None], width_sq[None])


def per_device(velocity, y_gap):
    width_sq = width_square(y_gap)
    inverse = 2.0 / (y_gap[:-1] + y_gap[1:])
    before_x, after_x = neighbours(velocity, GX, 1, HALO)
    before_z, after_z = neighbours(velocity, GZ, 2, HALO)
    rim = jnp.concatenate([before_x, after_x], axis=1)
    corner_before, corner_after = neighbours(rim, GZ, 2, HALO)
    halos = (before_x, after_x, before_z, after_z, corner_before, corner_after)
    lm_field, mm_field, strain_size, plane_pair = fields(velocity, halos, inverse, width_sq)
    planes = velocity.shape[1] * lax.axis_size(GX) * velocity.shape[2] * lax.axis_size(GZ)
    total_pair = over_axes(plane_pair)
    coefficient = total_pair[0] / planes / (total_pair[1] / planes + 1e-06)
    eddy_visc = coefficient * width_sq * strain_size
    return (eddy_visc, lm_field, mm_field, coefficient)


def solution(mesh):
    torus = Mesh(mesh.devices.reshape(8, 2, 4, 2, 2), ("gx_0", "gx_1", "gz_0", "gz_1", "gz_2"))
    return jax.shard_map(
        per_device,
        mesh=torus,
        in_specs=(P(None, GX, GZ, None), P()),
        out_specs=(P(GX, GZ, None), P(GX, GZ, None), P(GX, GZ, None), P()),
        check_vma=False,
    )
```

```python
import functools

import jax
import jax.numpy as jnp
from jax import lax
from jax.experimental import pallas as pl
from jax.experimental.pallas import tpu as pltpu
from jax.sharding import Mesh
from jax.sharding import PartitionSpec as P

GX = ("gx_0", "gx_1")
GZ = ("gz_0", "gz_1", "gz_2")

LANES = 128
SUB = 8
TOP = 8
HALO = 2


def exchange(last, leading, axis):
    size = lax.axis_size(axis)
    up = [(i, (i + 1) % size) for i in range(size)]
    down = [(j, i) for i, j in up]
    return lax.ppermute(last, axis, up), lax.ppermute(leading, axis, down)


def over_axes(copies):
    half = jnp.sum(lax.all_to_all(copies, ("gx_0", "gz_2"), 0, 0, tiled=True), axis=0)
    copies = jnp.broadcast_to(half[None], copies.shape)
    return jnp.sum(lax.all_to_all(copies, ("gx_1", "gz_0", "gz_1"), 0, 0, tiled=True), axis=0)


def width_square(y_gap):
    return (0.5 * (y_gap[:-1] + y_gap[1:])) ** (2.0 / 3.0)


def strain_of(ref, slopes, at, chunk, row):
    def cell(k, step_x=0, step_z=0):
        return ref[k, at + step_x, chunk, pl.ds(row + step_z, SUB), :]

    along_x = [cell(k, 1) - cell(k, -1) for k in range(3)]
    along_z = [cell(k, 0, 1) - cell(k, 0, -1) for k in range(3)]
    parts = [
        along_x[0],
        slopes[1],
        along_z[2],
        slopes[0] + along_x[1],
        along_z[0] + along_x[2],
        along_z[1] + slopes[2],
    ]
    squares = [part * part for part in parts]
    square = 0.5 * (squares[0] + squares[1] + squares[2]) + 0.25 * (
        squares[3] + squares[4] + squares[5]
    )
    return parts, jnp.sqrt(square)


def wall_slopes(read, inverse, chunks):
    lane = lax.broadcasted_iota(jnp.int32, (SUB, LANES), 1)
    values = [read(c) for c in range(chunks)]
    ahead = [pltpu.roll(value, LANES - 1, 1) for value in values] + [jnp.zeros_like(values[0])]
    behind = [jnp.zeros_like(values[0])] + [pltpu.roll(value, 1, 1) for value in values]
    return [
        (
            jnp.where(lane == LANES - 1, ahead[c + 1], ahead[c])
            - jnp.where(lane == 0, behind[c], behind[c + 1])
        )
        * inverse[c]
        for c in range(chunks)
    ]


PAIRS = ((0, 0), (1, 1), (2, 2), (0, 1), (0, 2), (1, 2))


def smooth(below, here, above):
    return (below + above) + (here + here)


def column(c):
    return slice(c * LANES, (c + 1) * LANES)


def put_layer(cells, at, rows, value):
    for k in range(3):
        for c in range(value(k).shape[-1] // LANES):
            cells[k, at, c, rows, :] = value(k)[:, column(c)]


def split_kernel(v_ref, first_x, last_x, first_z, last_z, cells):
    _, nx, nz, _ = v_ref.shape
    for k in range(3):
        for j in range(HALO):
            first_x[k, j] = v_ref[k, j]
            last_x[k, j] = v_ref[k, nx - HALO + j]
        for i in range(nx):
            first_z[k, i] = v_ref[k, i, :HALO, :]
            last_z[k, i] = v_ref[k, i, nz - HALO :, :]

    def own(i, carry):
        put_layer(cells, i + HALO, slice(TOP, TOP + nz), lambda k: v_ref[k, i])
        return carry

    lax.fori_loop(0, nx, own, 0)


def layer_pass(i, inverse, cells, filtered, smoothed, size_ref, sizes, products):
    chunks, nz = filtered.shape[2:4]
    nx = cells.shape[1] - 2 * HALO
    blocks = nz // SUB
    wide = [TOP - 1 + SUB * b for b in range(blocks + 1)]
    at = i + 1
    for row in wide:
        per_speed = [
            wall_slopes(lambda c: cells[k, at, c, pl.ds(row, SUB), :], inverse, chunks)
            for k in range(3)
        ]
        for c in range(chunks):
            parts, size = strain_of(cells, [per_speed[k][c] for k in range(3)], at, c, row)
            sizes[c, pl.ds(row, SUB), :] = size
            speeds = [cells[k, at, c, pl.ds(row, SUB), :] for k in range(3)]
            for n in range(6):
                products[n, c, pl.ds(row, SUB), :] = size * parts[n]
                p, q = PAIRS[n]
                products[6 + n, c, pl.ds(row, SUB), :] = speeds[p] * speeds[q]
    for c in range(chunks):
        for b in range(blocks):
            row = TOP + SUB * b
            for n in range(12):
                filtered[n, i, c, pl.ds(SUB * b, SUB), :] = smooth(
                    *[products[n, c, pl.ds(row + s, SUB), :] for s in (-1, 0, 1)]
                )

    @pl.when(jnp.logical_and(i >= 1, i <= nx))
    def _():
        for c in range(chunks):
            for b in range(blocks):
                size_ref[i - 1, SUB * b : SUB * (b + 1), column(c)] = sizes[
                    c, TOP + SUB * b : TOP + SUB * (b + 1), :
                ]

    for k in range(3):
        for c in range(chunks):
            for b in range(blocks + 2):
                row = SUB * b
                products[k, c, pl.ds(row, SUB), :] = smooth(
                    *[cells[k, at + s, c, pl.ds(row, SUB), :] for s in (-1, 0, 1)]
                )
            for row in wide:
                smoothed[k, i, c, pl.ds(row, SUB), :] = smooth(
                    *[products[k, c, pl.ds(row + s, SUB), :] for s in (-1, 0, 1)]
                )


def result_pass(i, inverse, width, filtered, smoothed, lm_ref, mm_ref, totals):
    chunks, nz = filtered.shape[2:4]
    at = i + 1
    add = functools.partial(functools.reduce, jnp.add)
    for b in range(nz // SUB):
        row = TOP + SUB * b
        per_speed = [
            wall_slopes(lambda c: smoothed[k, at, c, pl.ds(row, SUB), :], inverse, chunks)
            for k in range(3)
        ]
        for c in range(chunks):
            parts, size = strain_of(smoothed, [per_speed[k][c] for k in range(3)], at, c, row)
            size = 0.25 * size
            speeds = [0.25 * smoothed[k, at, c, pl.ds(row, SUB), :] for k in range(3)]

            def over_x(n):
                return smooth(*[filtered[n, i + s, c, pl.ds(SUB * b, SUB), :] for s in range(3)])

            cross, diagonal, outside = [], [], []
            for n in range(6):
                model = over_x(n) - size * parts[n]
                p, q = PAIRS[n]
                cross.append((over_x(6 + n) - speeds[p] * speeds[q]) * model)
                (diagonal if n < 3 else outside).append(model * model)
            lm = (width[c] * (1.0 / 256.0)) * add(cross)
            mm = (width[c] * width[c] * (1.0 / 256.0)) * (add(diagonal) + 0.5 * add(outside))
            lm_ref[i, SUB * b : SUB * (b + 1), column(c)] = lm
            mm_ref[i, SUB * b : SUB * (b + 1), column(c)] = mm
            totals[0, c] += lm
            totals[1, c] += mm


def rows_of(ref):
    return [
        jnp.broadcast_to(ref[:, column(c)], (SUB, LANES)) for c in range(ref.shape[-1] // LANES)
    ]


def inner_kernel(
    before_z, after_z, inv_ref, width_ref, cells_in,
    cells, filtered, smoothed, lm_ref, mm_ref, size_ref, totals,
    sizes, products,
):
    nx, nz, _ = lm_ref.shape

    def sides(i, carry):
        put_layer(cells, i + HALO, slice(TOP - HALO, TOP), lambda k: before_z[k, i])
        put_layer(cells, i + HALO, slice(TOP + nz, TOP + nz + HALO), lambda k: after_z[k, i])
        return carry

    lax.fori_loop(0, nx, sides, 0)
    inverse, width = rows_of(inv_ref), rows_of(width_ref)

    def layer(i, carry):
        layer_pass(i, inverse, cells, filtered, smoothed, size_ref, sizes, products)
        return carry

    lax.fori_loop(HALO, nx, layer, 0)
    totals[...] = jnp.zeros_like(totals)

    def result(i, carry):
        result_pass(i, inverse, width, filtered, smoothed, lm_ref, mm_ref, totals)
        return carry

    lax.fori_loop(HALO, nx - HALO, result, 0)


def outer_kernel(
    before_x, after_x, corner_before, corner_after, inv_ref, width_ref,
    cells_in, filtered_in, smoothed_in, lm_in, mm_in, size_in, totals_in,
    cells, filtered, smoothed, lm_ref, mm_ref, size_ref, totals, copies,
    sizes, products,
):
    nx, nz, _ = lm_ref.shape
    for j in range(HALO):
        for at, main, m in ((j, before_x, j), (nx + HALO + j, after_x, HALO + j)):
            put_layer(cells, at, slice(TOP, TOP + nz), lambda k: main[k, j])
            put_layer(cells, at, slice(TOP - HALO, TOP), lambda k: corner_before[k, m])
            put_layer(cells, at, slice(TOP + nz, TOP + nz + HALO), lambda k: corner_after[k, m])
    inverse, width = rows_of(inv_ref), rows_of(width_ref)

    def layer(j, carry):
        i = jnp.where(j < HALO, j, j + nx - HALO)
        layer_pass(i, inverse, cells, filtered, smoothed, size_ref, sizes, products)
        return carry

    lax.fori_loop(0, 2 * HALO, layer, 0)

    def result(j, carry):
        i = jnp.where(j < HALO, j, j + nx - 2 * HALO)
        result_pass(i, inverse, width, filtered, smoothed, lm_ref, mm_ref, totals)
        return carry

    lax.fori_loop(0, 2 * HALO, result, 0)
    for n in range(2):
        for c in range(totals.shape[1]):
            line = jnp.sum(totals[n, c], axis=0, keepdims=True)
            for member in range(copies.shape[0]):
                copies[member, n : n + 1, column(c)] = line


def call(kernel, outs, scratch, name, flops, aliases, args):
    whole = pl.BlockSpec(memory_space=pltpu.VMEM)
    return pl.pallas_call(
        kernel,
        out_shape=tuple(pltpu.VMEM(shape, jnp.float32) for shape in outs),
        in_specs=[whole] * len(args),
        out_specs=tuple([whole] * len(outs)),
        scratch_shapes=scratch,
        input_output_aliases=aliases,
        name=name,
        cost_estimate=pl.CostEstimate(flops=flops, bytes_accessed=0, transcendentals=0),
        compiler_params=pltpu.CompilerParams(vmem_limit_bytes=VMEM_LIMIT),
    )(*args)


VMEM_LIMIT = 16 * 2**20


def per_device(velocity, y_gap):
    _, nx, nz, ny = velocity.shape
    chunks, rows = ny // LANES, nz + 2 * SUB
    width_sq = width_square(y_gap)
    inverse = 2.0 / (y_gap[:-1] + y_gap[1:])
    lines = (inverse[None], width_sq[None])

    cells_shape = (3, nx + 2 * HALO, chunks, rows, LANES)
    field = (nx, nz, ny)
    first_x, last_x, first_z, last_z, cells = call(
        split_kernel,
        [(3, HALO, nz, ny)] * 2 + [(3, nx, HALO, ny)] * 2 + [cells_shape],
        [], "split", 0, {}, (velocity,),
    )
    before_z, after_z = exchange(last_z, first_z, GZ)
    before_x, after_x = exchange(last_x, first_x, GX)
    near = jnp.concatenate([before_z, after_z], axis=2)
    corners_before, corners_after = exchange(near[:, nx - HALO :], near[:, :HALO], GX)

    scratch = [
        pltpu.VMEM((chunks, rows, LANES), jnp.float32),
        pltpu.VMEM((12, chunks, rows, LANES), jnp.float32),
    ]
    state_shapes = [
        cells_shape,
        (12, nx + 2, chunks, nz, LANES),
        (3, nx + 2, chunks, rows, LANES),
        field, field, field,
        (2, chunks, SUB, LANES),
    ]
    state = call(
        inner_kernel, state_shapes, scratch, "inner", 20_000_000, {4: 0},
        (before_z, after_z, *lines, cells),
    )
    corners = jnp.concatenate([corners_before, corners_after], axis=1)
    *state, copies = call(
        outer_kernel, [*state_shapes, (16, 2, ny)], scratch, "outer", 20_000_000,
        {6 + n: n for n in range(7)},
        (before_x, after_x, corners[:, :, :HALO], corners[:, :, HALO:], *lines, *state),
    )
    lm_field, mm_field, strain_size = state[3:6]
    planes = nx * lax.axis_size(GX) * nz * lax.axis_size(GZ)
    total_pair = over_axes(copies)
    coefficient = total_pair[0] / planes / (total_pair[1] / planes + 1e-06)
    eddy_visc = coefficient * width_sq * strain_size
    return (eddy_visc, lm_field, mm_field, coefficient)


def solution(mesh):
    torus = Mesh(mesh.devices.reshape(8, 2, 4, 2, 2), ("gx_0", "gx_1", "gz_0", "gz_1", "gz_2"))
    return jax.shard_map(
        per_device,
        mesh=torus,
        in_specs=(P(None, GX, GZ, None), P()),
        out_specs=(P(GX, GZ, None), P(GX, GZ, None), P(GX, GZ, None), P()),
        check_vma=False,
    )
```

```python
import functools

import jax
import jax.numpy as jnp
from jax import lax
from jax.experimental import pallas as pl
from jax.experimental.pallas import tpu as pltpu
from jax.sharding import Mesh
from jax.sharding import PartitionSpec as P


GX = ("gx_0", "gx_1")
GZ = ("gz_0", "gz_1", "gz_2")

LANES = 128
SUB = 8
TOP = 8
HALO = 2
QUAD = 2 * HALO
EARLY = 16


def exchange(last, leading, axis):
    size = lax.axis_size(axis)
    up = [(i, (i + 1) % size) for i in range(size)]
    down = [(j, i) for i, j in up]
    before = lax.ppermute(last, axis, up)
    after = lax.ppermute(leading, axis, down)
    return before, after


def over_axes(copies):
    half = jnp.sum(lax.all_to_all(copies, ("gx_0", "gz_2"), 0, 0, tiled=True), axis=0)
    copies = jnp.broadcast_to(half[None], copies.shape)
    return lax.all_to_all(copies, ("gx_1", "gz_0", "gz_1"), 0, 0, tiled=True)


def width_square(y_gap):
    return (0.5 * (y_gap[:-1] + y_gap[1:])) ** (2.0 / 3.0)


def strain_of(ref, slopes, at, chunk, row):
    def cell(k, step_x=0, step_z=0):
        return ref[k, at + step_x, chunk, pl.ds(row + step_z, SUB), :]

    along_x = [cell(k, 1) - cell(k, -1) for k in range(3)]
    along_z = [cell(k, 0, 1) - cell(k, 0, -1) for k in range(3)]
    parts = [
        along_x[0],
        slopes[1],
        along_z[2],
        slopes[0] + along_x[1],
        along_z[0] + along_x[2],
        along_z[1] + slopes[2],
    ]
    squares = [part * part for part in parts]
    square = 0.5 * (squares[0] + squares[1] + squares[2]) + 0.25 * (
        squares[3] + squares[4] + squares[5]
    )
    return parts, jnp.sqrt(square)


def wall_slopes(read, inverse, chunks):
    lane = lax.broadcasted_iota(jnp.int32, (SUB, LANES), 1)
    values = [read(c) for c in range(chunks)]
    ahead = [pltpu.roll(value, LANES - 1, 1) for value in values] + [jnp.zeros_like(values[0])]
    behind = [jnp.zeros_like(values[0])] + [pltpu.roll(value, 1, 1) for value in values]
    return [
        (
            jnp.where(lane == LANES - 1, ahead[c + 1], ahead[c])
            - jnp.where(lane == 0, behind[c], behind[c + 1])
        )
        * inverse[c]
        for c in range(chunks)
    ]


PAIRS = ((0, 0), (1, 1), (2, 2), (0, 1), (0, 2), (1, 2))


def smooth(below, here, above):
    return (below + above) + (here + here)


def column(c):
    return slice(c * LANES, (c + 1) * LANES)


def put_layer(cells, at, rows, value):
    for k in range(3):
        for c in range(value(k).shape[-1] // LANES):
            cells[k, at, c, rows, :] = value(k)[:, column(c)]


def split_kernel(v_ref, first_early, last_early, first_late, last_late, first_z, last_z, cells):
    _, nx, nz, _ = v_ref.shape
    early = first_early.shape[2]
    for k in range(3):
        for j in range(HALO):
            for at, head, tail in ((j, first_early, first_late), (nx - HALO + j, last_early, last_late)):
                head[k, j] = v_ref[k, at, :early, :]
                for q in range(tail.shape[2]):
                    row = early + QUAD * q
                    tail[k, j, q] = v_ref[k, at, row : row + QUAD, :]
        for i in range(nx):
            first_z[k, i] = v_ref[k, i, :HALO, :]
            last_z[k, i] = v_ref[k, i, nz - HALO :, :]

    def own(i, carry):
        put_layer(cells, i + HALO, slice(TOP, TOP + nz), lambda k: v_ref[k, i])
        return carry

    lax.fori_loop(0, nx, own, 0)


def layer_pass(i, inverse, cells, filtered, smoothed, size_ref, sizes, products):
    chunks, nz = filtered.shape[2:4]
    nx = cells.shape[1] - 2 * HALO
    blocks = nz // SUB
    wide = [TOP - 1 + SUB * b for b in range(blocks + 1)]
    at = i + 1
    for row in wide:
        per_speed = [
            wall_slopes(lambda c: cells[k, at, c, pl.ds(row, SUB), :], inverse, chunks)
            for k in range(3)
        ]
        for c in range(chunks):
            parts, size = strain_of(cells, [per_speed[k][c] for k in range(3)], at, c, row)
            sizes[c, pl.ds(row, SUB), :] = size
            speeds = [cells[k, at, c, pl.ds(row, SUB), :] for k in range(3)]
            for n in range(6):
                products[n, c, pl.ds(row, SUB), :] = size * parts[n]
                p, q = PAIRS[n]
                products[6 + n, c, pl.ds(row, SUB), :] = speeds[p] * speeds[q]
    for c in range(chunks):
        for b in range(blocks):
            row = TOP + SUB * b
            for n in range(12):
                filtered[n, i, c, pl.ds(SUB * b, SUB), :] = smooth(
                    *[products[n, c, pl.ds(row + s, SUB), :] for s in (-1, 0, 1)]
                )

    @pl.when(jnp.logical_and(i >= 1, i <= nx))
    def _():
        for c in range(chunks):
            for b in range(blocks):
                size_ref[i - 1, SUB * b : SUB * (b + 1), column(c)] = sizes[
                    c, TOP + SUB * b : TOP + SUB * (b + 1), :
                ]

    for k in range(3):
        for c in range(chunks):
            for b in range(blocks + 2):
                row = SUB * b
                products[k, c, pl.ds(row, SUB), :] = smooth(
                    *[cells[k, at + s, c, pl.ds(row, SUB), :] for s in (-1, 0, 1)]
                )
            for row in wide:
                smoothed[k, i, c, pl.ds(row, SUB), :] = smooth(
                    *[products[k, c, pl.ds(row + s, SUB), :] for s in (-1, 0, 1)]
                )


def result_pass(i, inverse, width, filtered, smoothed, lm_ref, mm_ref, totals):
    chunks, nz = filtered.shape[2:4]
    at = i + 1
    add = functools.partial(functools.reduce, jnp.add)
    for b in range(nz // SUB):
        row = TOP + SUB * b
        per_speed = [
            wall_slopes(lambda c: smoothed[k, at, c, pl.ds(row, SUB), :], inverse, chunks)
            for k in range(3)
        ]
        for c in range(chunks):
            parts, size = strain_of(smoothed, [per_speed[k][c] for k in range(3)], at, c, row)
            size = 0.25 * size
            speeds = [0.25 * smoothed[k, at, c, pl.ds(row, SUB), :] for k in range(3)]

            def over_x(n):
                return smooth(*[filtered[n, i + s, c, pl.ds(SUB * b, SUB), :] for s in range(3)])

            cross, diagonal, outside = [], [], []
            for n in range(6):
                model = over_x(n) - size * parts[n]
                p, q = PAIRS[n]
                cross.append((over_x(6 + n) - speeds[p] * speeds[q]) * model)
                (diagonal if n < 3 else outside).append(model * model)
            lm = (width[c] * (1.0 / 256.0)) * add(cross)
            mm = (width[c] * width[c] * (1.0 / 256.0)) * (add(diagonal) + 0.5 * add(outside))
            lm_ref[i, SUB * b : SUB * (b + 1), column(c)] = lm
            mm_ref[i, SUB * b : SUB * (b + 1), column(c)] = mm
            totals[0, c] += lm
            totals[1, c] += mm


def rows_of(ref):
    return [
        jnp.broadcast_to(ref[:, column(c)], (SUB, LANES)) for c in range(ref.shape[-1] // LANES)
    ]


def inner_kernel(
    before_z, after_z, inv_ref, width_ref, cells_in,
    cells, filtered, smoothed, lm_ref, mm_ref, size_ref, totals,
    sizes, products,
):
    nx, nz, _ = lm_ref.shape

    def sides(i, carry):
        put_layer(cells, i + HALO, slice(TOP - HALO, TOP), lambda k: before_z[k, i])
        put_layer(cells, i + HALO, slice(TOP + nz, TOP + nz + HALO), lambda k: after_z[k, i])
        return carry

    lax.fori_loop(0, nx, sides, 0)
    inverse, width = rows_of(inv_ref), rows_of(width_ref)

    def layer(i, carry):
        layer_pass(i, inverse, cells, filtered, smoothed, size_ref, sizes, products)
        return carry

    lax.fori_loop(HALO, nx, layer, 0)
    totals[...] = jnp.zeros_like(totals)

    def result(i, carry):
        result_pass(i, inverse, width, filtered, smoothed, lm_ref, mm_ref, totals)
        return carry

    lax.fori_loop(HALO, nx - HALO, result, 0)


def outer_kernel(
    before_early, after_early, before_late, after_late, inv_ref, width_ref,
    cells_in, filtered_in, smoothed_in, lm_in, mm_in, size_in, totals_in,
    cells, filtered, smoothed, lm_ref, mm_ref, size_ref, totals, copies,
    sizes, products,
):
    nx, nz, _ = lm_ref.shape
    for j in range(HALO):
        for at, head, tail in ((j, before_early, before_late), (nx + HALO + j, after_early, after_late)):
            early, quads = head.shape[2], tail.shape[2] - 1
            put_layer(cells, at, slice(TOP, TOP + early), lambda k: head[k, j])
            for q in range(quads):
                row = TOP + early + QUAD * q
                put_layer(cells, at, slice(row, row + QUAD), lambda k: tail[k, j, q])
            put_layer(cells, at, slice(TOP - HALO, TOP), lambda k: tail[k, j, quads, :HALO, :])
            put_layer(cells, at, slice(TOP + nz, TOP + nz + HALO), lambda k: tail[k, j, quads, HALO:, :])
    inverse, width = rows_of(inv_ref), rows_of(width_ref)

    def layer(j, carry):
        i = jnp.where(j < HALO, j, j + nx - HALO)
        layer_pass(i, inverse, cells, filtered, smoothed, size_ref, sizes, products)
        return carry

    lax.fori_loop(0, 2 * HALO, layer, 0)

    def result(j, carry):
        i = jnp.where(j < HALO, j, j + nx - 2 * HALO)
        result_pass(i, inverse, width, filtered, smoothed, lm_ref, mm_ref, totals)
        return carry

    lax.fori_loop(0, 2 * HALO, result, 0)
    for n in range(2):
        for c in range(totals.shape[1]):
            line = jnp.sum(totals[n, c], axis=0, keepdims=True)
            for member in range(copies.shape[0]):
                copies[member, n : n + 1, column(c)] = line


def finish_kernel(
    planes, parts_ref, width_ref, lm_ref, mm_ref, size_ref,
    eddy_out, lm_out, mm_out, coefficient_ref,
    eddy_ref, sems,
):
    stores = [
        pltpu.make_async_copy(lm_ref, lm_out, sems.at[0]),
        pltpu.make_async_copy(mm_ref, mm_out, sems.at[1]),
        pltpu.make_async_copy(eddy_ref, eddy_out, sems.at[2]),
    ]
    stores[0].start()
    stores[1].start()
    total = parts_ref[0]
    for member in range(1, parts_ref.shape[0]):
        total = total + parts_ref[member]
    coefficient = total[0:1] / planes / (total[1:2] / planes + 1e-06)
    coefficient_ref[...] = coefficient[0]
    eddy_ref[...] = (coefficient * width_ref[...])[None] * size_ref[...]
    stores[2].start()
    for store in stores:
        store.wait()


def call(kernel, outs, scratch, flops, aliases, args):
    whole = pl.BlockSpec(memory_space=pltpu.VMEM)
    return pl.pallas_call(
        kernel,
        out_shape=tuple(pltpu.VMEM(shape, jnp.float32) for shape in outs),
        in_specs=[whole] * len(args),
        out_specs=tuple([whole] * len(outs)),
        scratch_shapes=scratch,
        input_output_aliases=aliases,
        cost_estimate=pl.CostEstimate(flops=flops, bytes_accessed=0, transcendentals=0),
        compiler_params=pltpu.CompilerParams(vmem_limit_bytes=VMEM_LIMIT),
    )(*args)


VMEM_LIMIT = 16 * 2**20


def per_device(velocity, y_gap):
    _, nx, nz, ny = velocity.shape
    chunks, rows = ny // LANES, nz + 2 * SUB
    width_sq = width_square(y_gap)
    inverse = 2.0 / (y_gap[:-1] + y_gap[1:])
    lines = (inverse[None], width_sq[None])

    cells_shape = (3, nx + 2 * HALO, chunks, rows, LANES)
    field = (nx, nz, ny)
    quads = (nz - EARLY) // QUAD
    first_early, last_early, first_late, last_late, first_z, last_z, cells = call(
        split_kernel,
        [(3, HALO, EARLY, ny)] * 2 + [(3, HALO, quads, QUAD, ny)] * 2 + [(3, nx, HALO, ny)] * 2
        + [cells_shape],
        [], 0, {}, (velocity,),
    )
    before_z, after_z = exchange(last_z, first_z, GZ)
    before_early, after_early = exchange(last_early, first_early, GX)
    near = jnp.concatenate([before_z, after_z], axis=2)[:, :, None]
    before_late, after_late = exchange(
        jnp.concatenate([last_late, near[:, nx - HALO :]], axis=2),
        jnp.concatenate([first_late, near[:, :HALO]], axis=2),
        GX,
    )

    scratch = [
        pltpu.VMEM((chunks, rows, LANES), jnp.float32),
        pltpu.VMEM((12, chunks, rows, LANES), jnp.float32),
    ]
    state_shapes = [
        cells_shape,
        (12, nx + 2, chunks, nz, LANES),
        (3, nx + 2, chunks, rows, LANES),
        field, field, field,
        (2, chunks, SUB, LANES),
    ]
    state = call(
        inner_kernel, state_shapes, scratch, 20_000_000, {4: 0},
        (before_z, after_z, *lines, cells),
    )
    *state, copies = call(
        outer_kernel, [*state_shapes, (16, 2, ny)], scratch, 20_000_000,
        {6 + n: n for n in range(7)},
        (before_early, after_early, before_late, after_late, *lines, *state),
    )
    lm_field, mm_field, strain_size = state[3:6]
    planes = nx * lax.axis_size(GX) * nz * lax.axis_size(GZ)
    whole, there = pl.BlockSpec(memory_space=pltpu.VMEM), pl.BlockSpec(memory_space=pl.ANY)
    block = jax.ShapeDtypeStruct(field, jnp.float32)
    eddy_visc, lm_field, mm_field, coefficient = pl.pallas_call(
        functools.partial(finish_kernel, planes),
        out_shape=(block, block, block, jax.ShapeDtypeStruct((ny,), jnp.float32)),
        in_specs=[whole] * 5,
        out_specs=(there, there, there, whole),
        scratch_shapes=[pltpu.VMEM(field, jnp.float32), pltpu.SemaphoreType.DMA((3,))],
        name="finish",
        compiler_params=pltpu.CompilerParams(vmem_limit_bytes=VMEM_LIMIT),
    )(over_axes(copies), lines[1], lm_field, mm_field, strain_size)
    return (eddy_visc, lm_field, mm_field, coefficient)


def solution(mesh):
    torus = Mesh(mesh.devices.reshape(8, 2, 4, 2, 2), ("gx_0", "gx_1", "gz_0", "gz_1", "gz_2"))

    return jax.shard_map(
        per_device,
        mesh=torus,
        in_specs=(P(None, GX, GZ, None), P()),
        out_specs=(P(GX, GZ, None), P(GX, GZ, None), P(GX, GZ, None), P()),
        check_vma=False,
    )
```

```python
import functools

import jax
import jax.numpy as jnp
from jax import lax
from jax.experimental import pallas as pl
from jax.experimental.pallas import tpu as pltpu
from jax.sharding import Mesh
from jax.sharding import PartitionSpec as P


GX = ("gx_0", "gx_1")
GZ = ("gz_0", "gz_1", "gz_2")

LANES = 128
SUB = 8
TOP = 8
HALO = 2
EARLY_UP, EARLY_DOWN = 16, 16
QUAD = 2 * HALO


def send(array, axis, step):
    size = lax.axis_size(axis)
    return lax.ppermute(array, axis, [(i, (i + step) % size) for i in range(size)])


GROUPS = (("gx_1", "gz_0", "gz_1", "gz_2"), ("gx_0",))


def members(axes):
    return functools.reduce(lambda count, axis: count * lax.axis_size(axis), axes, 1)


def over_axes(copies):
    half = jnp.sum(lax.all_to_all(copies, GROUPS[0], 0, 0, tiled=True), axis=0)
    copies = jnp.broadcast_to(half[None], (members(GROUPS[1]), *half.shape))
    return lax.all_to_all(copies, GROUPS[1], 0, 0, tiled=True)


def width_square(y_gap):
    return (0.5 * (y_gap[:-1] + y_gap[1:])) ** (2.0 / 3.0)


def strain_of(ref, slopes, at, chunk, row):
    def cell(k, step_x=0, step_z=0):
        return ref[k, at + step_x, chunk, pl.ds(row + step_z, SUB), :]

    along_x = [cell(k, 1) - cell(k, -1) for k in range(3)]
    along_z = [cell(k, 0, 1) - cell(k, 0, -1) for k in range(3)]
    parts = [
        along_x[0],
        slopes[1],
        along_z[2],
        slopes[0] + along_x[1],
        along_z[0] + along_x[2],
        along_z[1] + slopes[2],
    ]
    squares = [part * part for part in parts]
    square = 0.5 * (squares[0] + squares[1] + squares[2]) + 0.25 * (
        squares[3] + squares[4] + squares[5]
    )
    return parts, jnp.sqrt(square)


def wall_slopes(read, inverse, chunks):
    lane = lax.broadcasted_iota(jnp.int32, (SUB, LANES), 1)
    values = [read(c) for c in range(chunks)]
    ahead = [pltpu.roll(value, LANES - 1, 1) for value in values] + [jnp.zeros_like(values[0])]
    behind = [jnp.zeros_like(values[0])] + [pltpu.roll(value, 1, 1) for value in values]
    return [
        (
            jnp.where(lane == LANES - 1, ahead[c + 1], ahead[c])
            - jnp.where(lane == 0, behind[c], behind[c + 1])
        )
        * inverse[c]
        for c in range(chunks)
    ]


PAIRS = ((0, 0), (1, 1), (2, 2), (0, 1), (0, 2), (1, 2))


def smooth(below, here, above):
    return (below + above) + (here + here)


def column(c):
    return slice(c * LANES, (c + 1) * LANES)


def put_layer(cells, at, rows, value):
    for k in range(3):
        for c in range(value(k).shape[-1] // LANES):
            cells[k, at, c, rows, :] = value(k)[:, column(c)]


def split_kernel(v_ref, first_early, last_early, first_late, last_late, first_z, last_z, cells):
    _, nx, nz, _ = v_ref.shape
    for k in range(3):
        for j in range(HALO):
            for at, head, tail in ((j, first_early, first_late), (nx - HALO + j, last_early, last_late)):
                early = head.shape[2]
                head[k, j] = v_ref[k, at, :early, :]
                for q in range(tail.shape[2]):
                    row = early + QUAD * q
                    tail[k, j, q] = v_ref[k, at, row : row + QUAD, :]
        for i in range(nx):
            first_z[k, i] = v_ref[k, i, :HALO, :]
            last_z[k, i] = v_ref[k, i, nz - HALO :, :]

    def own(i, carry):
        put_layer(cells, i + HALO, slice(TOP, TOP + nz), lambda k: v_ref[k, i])
        return carry

    lax.fori_loop(0, nx, own, 0)


def layer_pass(i, inverse, cells, filtered, smoothed, size_ref, sizes, products):
    chunks, nz = filtered.shape[2:4]
    nx = cells.shape[1] - 2 * HALO
    blocks = nz // SUB
    wide = [TOP - 1 + SUB * b for b in range(blocks + 1)]
    at = i + 1
    for row in wide:
        per_speed = [
            wall_slopes(lambda c: cells[k, at, c, pl.ds(row, SUB), :], inverse, chunks)
            for k in range(3)
        ]
        for c in range(chunks):
            parts, size = strain_of(cells, [per_speed[k][c] for k in range(3)], at, c, row)
            sizes[c, pl.ds(row, SUB), :] = size
            speeds = [cells[k, at, c, pl.ds(row, SUB), :] for k in range(3)]
            for n in range(6):
                products[n, c, pl.ds(row, SUB), :] = size * parts[n]
                p, q = PAIRS[n]
                products[6 + n, c, pl.ds(row, SUB), :] = speeds[p] * speeds[q]
    for c in range(chunks):
        for b in range(blocks):
            row = TOP + SUB * b
            for n in range(12):
                filtered[n, i, c, pl.ds(SUB * b, SUB), :] = smooth(
                    *[products[n, c, pl.ds(row + s, SUB), :] for s in (-1, 0, 1)]
                )

    @pl.when(jnp.logical_and(i >= 1, i <= nx))
    def _():
        for c in range(chunks):
            for b in range(blocks):
                size_ref[i - 1, SUB * b : SUB * (b + 1), column(c)] = sizes[
                    c, TOP + SUB * b : TOP + SUB * (b + 1), :
                ]

    for k in range(3):
        for c in range(chunks):
            for b in range(blocks + 2):
                row = SUB * b
                products[k, c, pl.ds(row, SUB), :] = smooth(
                    *[cells[k, at + s, c, pl.ds(row, SUB), :] for s in (-1, 0, 1)]
                )
            for row in wide:
                smoothed[k, i, c, pl.ds(row, SUB), :] = smooth(
                    *[products[k, c, pl.ds(row + s, SUB), :] for s in (-1, 0, 1)]
                )


def result_pass(i, inverse, width, filtered, smoothed, lm_ref, mm_ref, totals):
    chunks, nz = filtered.shape[2:4]
    at = i + 1
    add = functools.partial(functools.reduce, jnp.add)
    for b in range(nz // SUB):
        row = TOP + SUB * b
        per_speed = [
            wall_slopes(lambda c: smoothed[k, at, c, pl.ds(row, SUB), :], inverse, chunks)
            for k in range(3)
        ]
        for c in range(chunks):
            parts, size = strain_of(smoothed, [per_speed[k][c] for k in range(3)], at, c, row)
            size = 0.25 * size
            speeds = [0.25 * smoothed[k, at, c, pl.ds(row, SUB), :] for k in range(3)]

            def over_x(n):
                return smooth(*[filtered[n, i + s, c, pl.ds(SUB * b, SUB), :] for s in range(3)])

            cross, diagonal, outside = [], [], []
            for n in range(6):
                model = over_x(n) - size * parts[n]
                p, q = PAIRS[n]
                cross.append((over_x(6 + n) - speeds[p] * speeds[q]) * model)
                (diagonal if n < 3 else outside).append(model * model)
            lm = (width[c] * (1.0 / 256.0)) * add(cross)
            mm = (width[c] * width[c] * (1.0 / 256.0)) * (add(diagonal) + 0.5 * add(outside))
            lm_ref[i, SUB * b : SUB * (b + 1), column(c)] = lm
            mm_ref[i, SUB * b : SUB * (b + 1), column(c)] = mm
            totals[0, c] += lm
            totals[1, c] += mm


def rows_of(ref):
    return [
        jnp.broadcast_to(ref[:, column(c)], (SUB, LANES)) for c in range(ref.shape[-1] // LANES)
    ]


def inner_kernel(
    before_z, after_z, inv_ref, width_ref, cells_in,
    cells, filtered, smoothed, lm_ref, mm_ref, size_ref, totals,
    sizes, products,
):
    nx, nz, _ = lm_ref.shape

    def sides(i, carry):
        put_layer(cells, i + HALO, slice(TOP - HALO, TOP), lambda k: before_z[k, i])
        put_layer(cells, i + HALO, slice(TOP + nz, TOP + nz + HALO), lambda k: after_z[k, i])
        return carry

    lax.fori_loop(0, nx, sides, 0)
    inverse, width = rows_of(inv_ref), rows_of(width_ref)

    def layer(i, carry):
        layer_pass(i, inverse, cells, filtered, smoothed, size_ref, sizes, products)
        return carry

    lax.fori_loop(HALO, nx, layer, 0)
    totals[...] = jnp.zeros_like(totals)

    def result(i, carry):
        result_pass(i, inverse, width, filtered, smoothed, lm_ref, mm_ref, totals)
        return carry

    lax.fori_loop(HALO, nx - HALO, result, 0)


STATE = 7


def outer_pass(layers, inv_ref, width_ref, state, scratch):
    cells, filtered, smoothed, lm_ref, mm_ref, size_ref, totals = state
    inverse, width = rows_of(inv_ref), rows_of(width_ref)

    def layer(j, carry):
        layer_pass(layers[0] + j, inverse, cells, filtered, smoothed, size_ref, *scratch)
        return carry

    lax.fori_loop(0, HALO, layer, 0, unroll=True)

    def result(j, carry):
        result_pass(layers[1] + j, inverse, width, filtered, smoothed, lm_ref, mm_ref, totals)
        return carry

    lax.fori_loop(0, HALO, result, 0, unroll=True)


def fill_rim(cells, at, early, late):
    head, quads = early.shape[2], late.shape[2] - 1
    end = TOP + head + QUAD * quads
    for j in range(HALO):
        put_layer(cells, at + j, slice(TOP, TOP + head), lambda k: early[k, j])
        for q in range(quads):
            row = TOP + head + QUAD * q
            put_layer(cells, at + j, slice(row, row + QUAD), lambda k: late[k, j, q])
        put_layer(cells, at + j, slice(TOP - HALO, TOP), lambda k: late[k, j, quads, :HALO, :])
        put_layer(cells, at + j, slice(end, end + HALO), lambda k: late[k, j, quads, HALO:, :])


def low_kernel(early, late, inv_ref, width_ref, *refs):
    state, scratch = refs[STATE : 2 * STATE], refs[2 * STATE :]
    fill_rim(state[0], 0, early, late)
    outer_pass((0, 0), inv_ref, width_ref, state, scratch)


def high_kernel(early, late, inv_ref, width_ref, *refs):
    state, copies, scratch = refs[STATE : 2 * STATE], refs[2 * STATE], refs[2 * STATE + 1 :]
    nx = state[3].shape[0]
    totals = state[6]
    fill_rim(state[0], nx + HALO, early, late)
    outer_pass((nx, nx - HALO), inv_ref, width_ref, state, scratch)
    for n in range(2):
        for c in range(totals.shape[1]):
            line = jnp.sum(totals[n, c], axis=0, keepdims=True)
            for member in range(copies.shape[0]):
                copies[member, n : n + 1, column(c)] = line


def finish_kernel(
    planes, parts_ref, width_ref, lm_ref, mm_ref, size_ref,
    eddy_out, lm_out, mm_out, coefficient_ref,
    eddy_ref, sems,
):
    stores = [
        pltpu.make_async_copy(lm_ref, lm_out, sems.at[0]),
        pltpu.make_async_copy(mm_ref, mm_out, sems.at[1]),
        pltpu.make_async_copy(eddy_ref, eddy_out, sems.at[2]),
    ]
    stores[0].start()
    stores[1].start()
    total = parts_ref[0]
    for member in range(1, parts_ref.shape[0]):
        total = total + parts_ref[member]
    coefficient = total[0:1] / planes / (total[1:2] / planes + 1e-06)
    coefficient_ref[...] = coefficient[0]
    eddy_ref[...] = (coefficient * width_ref[...])[None] * size_ref[...]
    stores[2].start()
    for store in stores:
        store.wait()


def call(kernel, outs, scratch, flops, aliases, args):
    whole = pl.BlockSpec(memory_space=pltpu.VMEM)
    return pl.pallas_call(
        kernel,
        out_shape=tuple(pltpu.VMEM(shape, jnp.float32) for shape in outs),
        in_specs=[whole] * len(args),
        out_specs=tuple([whole] * len(outs)),
        scratch_shapes=scratch,
        input_output_aliases=aliases,
        cost_estimate=pl.CostEstimate(flops=flops, bytes_accessed=0, transcendentals=0),
        compiler_params=pltpu.CompilerParams(vmem_limit_bytes=VMEM_LIMIT),
    )(*args)


VMEM_LIMIT = 16 * 2**20


def per_device(velocity, y_gap):
    _, nx, nz, ny = velocity.shape
    chunks, rows = ny // LANES, nz + 2 * SUB
    width_sq = width_square(y_gap)
    inverse = 2.0 / (y_gap[:-1] + y_gap[1:])
    lines = (inverse[None], width_sq[None])

    cells_shape = (3, nx + 2 * HALO, chunks, rows, LANES)
    field = (nx, nz, ny)
    early = (EARLY_DOWN, EARLY_UP)
    first_early, last_early, first_late, last_late, first_z, last_z, cells = call(
        split_kernel,
        [(3, HALO, e, ny) for e in early] + [(3, HALO, (nz - e) // QUAD, QUAD, ny) for e in early]
        + [(3, nx, HALO, ny)] * 2
        + [cells_shape],
        [], 0, {}, (velocity,),
    )
    before_z = send(last_z, GZ, 1)
    after_z = send(first_z, GZ, -1)
    before_early = send(last_early, GX, 1)
    after_early = send(first_early, GX, -1)
    near = jnp.concatenate([before_z, after_z], axis=2)[:, :, None]
    last_late = jnp.concatenate([last_late, near[:, nx - HALO :]], axis=2)
    first_late = jnp.concatenate([first_late, near[:, :HALO]], axis=2)
    before_late = send(last_late, GX, 1)
    after_late = send(first_late, GX, -1)

    scratch = [
        pltpu.VMEM((chunks, rows, LANES), jnp.float32),
        pltpu.VMEM((12, chunks, rows, LANES), jnp.float32),
    ]
    state_shapes = [
        cells_shape,
        (12, nx + 2, chunks, nz, LANES),
        (3, nx + 2, chunks, rows, LANES),
        field, field, field,
        (2, chunks, SUB, LANES),
    ]
    state = call(
        inner_kernel, state_shapes, scratch, 20_000_000, {4: 0},
        (before_z, after_z, *lines, cells),
    )
    state = call(
        low_kernel, state_shapes, scratch, 10_000_000,
        {4 + n: n for n in range(STATE)}, (before_early, before_late, *lines, *state),
    )
    *state, copies = call(
        high_kernel, [*state_shapes, (members(GROUPS[0]), 2, ny)], scratch, 10_000_000,
        {4 + n: n for n in range(STATE)}, (after_early, after_late, *lines, *state),
    )
    lm_field, mm_field, strain_size = state[3:6]
    planes = nx * lax.axis_size(GX) * nz * lax.axis_size(GZ)
    whole, there = pl.BlockSpec(memory_space=pltpu.VMEM), pl.BlockSpec(memory_space=pl.ANY)
    block = jax.ShapeDtypeStruct(field, jnp.float32)
    eddy_visc, lm_field, mm_field, coefficient = pl.pallas_call(
        functools.partial(finish_kernel, planes),
        out_shape=(block, block, block, jax.ShapeDtypeStruct((ny,), jnp.float32)),
        in_specs=[whole] * 5,
        out_specs=(there, there, there, whole),
        scratch_shapes=[pltpu.VMEM(field, jnp.float32), pltpu.SemaphoreType.DMA((3,))],
        name="finish",
        compiler_params=pltpu.CompilerParams(vmem_limit_bytes=VMEM_LIMIT),
    )(over_axes(copies), lines[1], lm_field, mm_field, strain_size)
    return (eddy_visc, lm_field, mm_field, coefficient)


def solution(mesh):
    torus = Mesh(mesh.devices.reshape(8, 2, 4, 2, 2), ("gx_0", "gx_1", "gz_0", "gz_1", "gz_2"))

    return jax.shard_map(
        per_device,
        mesh=torus,
        in_specs=(P(None, GX, GZ, None), P()),
        out_specs=(P(GX, GZ, None), P(GX, GZ, None), P(GX, GZ, None), P()),
        check_vma=False,
    )
```

```python
import functools

import jax
import jax.numpy as jnp
from jax import lax
from jax.experimental import pallas as pl
from jax.experimental.pallas import tpu as pltpu
from jax.sharding import Mesh
from jax.sharding import PartitionSpec as P


GX = ("gx_0", "gx_1")
GZ = ("gz_0", "gz_1", "gz_2")

LANES = 128
SUB = 8
TOP = 8
HALO = 2
EARLY_UP, EARLY_DOWN = 24, 24
QUAD = 2 * HALO


def send(array, axis, target):
    size = lax.axis_size(axis)
    return lax.ppermute(array, axis, [(i, target(i) % size) for i in range(size)])


def is_odd():
    return lax.axis_index("gz_2") == 1


def pick(odd, if_odd, if_even):
    return jnp.where(odd, if_odd, if_even)


GROUPS = (("gx_1", "gz_0", "gz_1", "gz_2"), ("gx_0",))


def members(axes):
    return functools.reduce(lambda count, axis: count * lax.axis_size(axis), axes, 1)


def over_axes(copies):
    half = jnp.sum(lax.all_to_all(copies, GROUPS[0], 0, 0, tiled=True), axis=0)
    copies = jnp.broadcast_to(half[None], (members(GROUPS[1]), *half.shape))
    return lax.all_to_all(copies, GROUPS[1], 0, 0, tiled=True)


def width_square(y_gap):
    return (0.5 * (y_gap[:-1] + y_gap[1:])) ** (2.0 / 3.0)


def strain_of(ref, slopes, at, chunk, row):
    def cell(k, step_x=0, step_z=0):
        return ref[k, at + step_x, chunk, pl.ds(row + step_z, SUB), :]

    along_x = [cell(k, 1) - cell(k, -1) for k in range(3)]
    along_z = [cell(k, 0, 1) - cell(k, 0, -1) for k in range(3)]
    parts = [
        along_x[0],
        slopes[1],
        along_z[2],
        slopes[0] + along_x[1],
        along_z[0] + along_x[2],
        along_z[1] + slopes[2],
    ]
    squares = [part * part for part in parts]
    square = 0.5 * (squares[0] + squares[1] + squares[2]) + 0.25 * (
        squares[3] + squares[4] + squares[5]
    )
    return parts, jnp.sqrt(square)


def wall_slopes(read, inverse, chunks):
    lane = lax.broadcasted_iota(jnp.int32, (SUB, LANES), 1)
    values = [read(c) for c in range(chunks)]
    ahead = [pltpu.roll(value, LANES - 1, 1) for value in values] + [jnp.zeros_like(values[0])]
    behind = [jnp.zeros_like(values[0])] + [pltpu.roll(value, 1, 1) for value in values]
    return [
        (
            jnp.where(lane == LANES - 1, ahead[c + 1], ahead[c])
            - jnp.where(lane == 0, behind[c], behind[c + 1])
        )
        * inverse[c]
        for c in range(chunks)
    ]


PAIRS = ((0, 0), (1, 1), (2, 2), (0, 1), (0, 2), (1, 2))


def smooth(below, here, above):
    return (below + above) + (here + here)


def column(c):
    return slice(c * LANES, (c + 1) * LANES)


def put_layer(cells, at, rows, value):
    for k in range(3):
        for c in range(value(k).shape[-1] // LANES):
            cells[k, at, c, rows, :] = value(k)[:, column(c)]


def split_kernel(v_ref, first_early, last_early, first_late, last_late, across, within, cells):
    _, nx, nz, _ = v_ref.shape
    odd = is_odd()
    for k in range(3):
        for j in range(HALO):
            for at, head, tail in ((j, first_early, first_late), (nx - HALO + j, last_early, last_late)):
                early = head.shape[2]
                head[k, j] = v_ref[k, at, :early, :]
                for q in range(tail.shape[2]):
                    row = early + QUAD * q
                    tail[k, j, q] = v_ref[k, at, row : row + QUAD, :]
        for i in range(nx):
            first, last = v_ref[k, i, :HALO, :], v_ref[k, i, nz - HALO :, :]
            across[k, i] = pick(odd, last, first)
            within[k, i] = pick(odd, first, last)

    def own(i, carry):
        put_layer(cells, i + HALO, slice(TOP, TOP + nz), lambda k: v_ref[k, i])
        return carry

    lax.fori_loop(0, nx, own, 0)


def join_kernel(across, within, first_late, last_late, first_out, last_out):
    nx = across.shape[1]
    odd = is_odd()
    for k in range(3):
        for j in range(HALO):
            for at, late, out in ((j, first_late, first_out), (nx - HALO + j, last_late, last_out)):
                quads = late.shape[2]
                for q in range(quads):
                    out[k, j, q] = late[k, j, q]
                there, here = across[k, at], within[k, at]
                out[k, j, quads, :HALO, :] = pick(odd, here, there)
                out[k, j, quads, HALO:, :] = pick(odd, there, here)


def layer_pass(i, inverse, cells, filtered, smoothed, size_ref, sizes, products):
    chunks, nz = filtered.shape[2:4]
    nx = cells.shape[1] - 2 * HALO
    blocks = nz // SUB
    wide = [TOP - 1 + SUB * b for b in range(blocks + 1)]
    at = i + 1
    for row in wide:
        per_speed = [
            wall_slopes(lambda c: cells[k, at, c, pl.ds(row, SUB), :], inverse, chunks)
            for k in range(3)
        ]
        for c in range(chunks):
            parts, size = strain_of(cells, [per_speed[k][c] for k in range(3)], at, c, row)
            sizes[c, pl.ds(row, SUB), :] = size
            speeds = [cells[k, at, c, pl.ds(row, SUB), :] for k in range(3)]
            for n in range(6):
                products[n, c, pl.ds(row, SUB), :] = size * parts[n]
                p, q = PAIRS[n]
                products[6 + n, c, pl.ds(row, SUB), :] = speeds[p] * speeds[q]
    for c in range(chunks):
        for b in range(blocks):
            row = TOP + SUB * b
            for n in range(12):
                filtered[n, i, c, pl.ds(SUB * b, SUB), :] = smooth(
                    *[products[n, c, pl.ds(row + s, SUB), :] for s in (-1, 0, 1)]
                )

    @pl.when(jnp.logical_and(i >= 1, i <= nx))
    def _():
        for c in range(chunks):
            for b in range(blocks):
                size_ref[i - 1, SUB * b : SUB * (b + 1), column(c)] = sizes[
                    c, TOP + SUB * b : TOP + SUB * (b + 1), :
                ]

    for k in range(3):
        for c in range(chunks):
            for b in range(blocks + 2):
                row = SUB * b
                products[k, c, pl.ds(row, SUB), :] = smooth(
                    *[cells[k, at + s, c, pl.ds(row, SUB), :] for s in (-1, 0, 1)]
                )
            for row in wide:
                smoothed[k, i, c, pl.ds(row, SUB), :] = smooth(
                    *[products[k, c, pl.ds(row + s, SUB), :] for s in (-1, 0, 1)]
                )


def result_pass(i, inverse, width, filtered, smoothed, lm_ref, mm_ref, totals):
    chunks, nz = filtered.shape[2:4]
    at = i + 1
    add = functools.partial(functools.reduce, jnp.add)
    for b in range(nz // SUB):
        row = TOP + SUB * b
        per_speed = [
            wall_slopes(lambda c: smoothed[k, at, c, pl.ds(row, SUB), :], inverse, chunks)
            for k in range(3)
        ]
        for c in range(chunks):
            parts, size = strain_of(smoothed, [per_speed[k][c] for k in range(3)], at, c, row)
            size = 0.25 * size
            speeds = [0.25 * smoothed[k, at, c, pl.ds(row, SUB), :] for k in range(3)]

            def over_x(n):
                return smooth(*[filtered[n, i + s, c, pl.ds(SUB * b, SUB), :] for s in range(3)])

            cross, diagonal, outside = [], [], []
            for n in range(6):
                model = over_x(n) - size * parts[n]
                p, q = PAIRS[n]
                cross.append((over_x(6 + n) - speeds[p] * speeds[q]) * model)
                (diagonal if n < 3 else outside).append(model * model)
            lm = (width[c] * (1.0 / 256.0)) * add(cross)
            mm = (width[c] * width[c] * (1.0 / 256.0)) * (add(diagonal) + 0.5 * add(outside))
            lm_ref[i, SUB * b : SUB * (b + 1), column(c)] = lm
            mm_ref[i, SUB * b : SUB * (b + 1), column(c)] = mm
            totals[0, c] += lm
            totals[1, c] += mm


def rows_of(ref):
    return [
        jnp.broadcast_to(ref[:, column(c)], (SUB, LANES)) for c in range(ref.shape[-1] // LANES)
    ]


def inner_kernel(
    across, within, inv_ref, width_ref, cells_in,
    cells, filtered, smoothed, lm_ref, mm_ref, size_ref, totals,
    sizes, products,
):
    nx, nz, _ = lm_ref.shape

    odd = is_odd()

    def sides(i, carry):
        for rows, flip in ((slice(TOP - HALO, TOP), False), (slice(TOP + nz, TOP + nz + HALO), True)):
            there, here = (across, within) if flip else (within, across)
            put_layer(cells, i + HALO, rows, lambda k: pick(odd, there[k, i], here[k, i]))
        return carry

    lax.fori_loop(0, nx, sides, 0)
    inverse, width = rows_of(inv_ref), rows_of(width_ref)

    def layer(i, carry):
        layer_pass(i, inverse, cells, filtered, smoothed, size_ref, sizes, products)
        return carry

    lax.fori_loop(HALO, nx, layer, 0)
    totals[...] = jnp.zeros_like(totals)

    def result(i, carry):
        result_pass(i, inverse, width, filtered, smoothed, lm_ref, mm_ref, totals)
        return carry

    lax.fori_loop(HALO, nx - HALO, result, 0)


STATE = 7


def outer_pass(layers, inv_ref, width_ref, state, scratch):
    cells, filtered, smoothed, lm_ref, mm_ref, size_ref, totals = state
    inverse, width = rows_of(inv_ref), rows_of(width_ref)

    def layer(j, carry):
        layer_pass(layers[0] + j, inverse, cells, filtered, smoothed, size_ref, *scratch)
        return carry

    lax.fori_loop(0, HALO, layer, 0, unroll=True)

    def result(j, carry):
        result_pass(layers[1] + j, inverse, width, filtered, smoothed, lm_ref, mm_ref, totals)
        return carry

    lax.fori_loop(0, HALO, result, 0, unroll=True)


def fill_rim(cells, at, early, late):
    head, quads = early.shape[2], late.shape[2] - 1
    end = TOP + head + QUAD * quads
    for j in range(HALO):
        put_layer(cells, at + j, slice(TOP, TOP + head), lambda k: early[k, j])
        for q in range(quads):
            row = TOP + head + QUAD * q
            put_layer(cells, at + j, slice(row, row + QUAD), lambda k: late[k, j, q])
        put_layer(cells, at + j, slice(TOP - HALO, TOP), lambda k: late[k, j, quads, :HALO, :])
        put_layer(cells, at + j, slice(end, end + HALO), lambda k: late[k, j, quads, HALO:, :])


def low_kernel(early, late, inv_ref, width_ref, *refs):
    state, scratch = refs[STATE : 2 * STATE], refs[2 * STATE :]
    fill_rim(state[0], 0, early, late)
    outer_pass((0, 0), inv_ref, width_ref, state, scratch)


def high_kernel(early, late, inv_ref, width_ref, *refs):
    state, (copies, lm_out, mm_out, *scratch, sems) = refs[STATE : 2 * STATE], refs[2 * STATE :]
    nx = state[3].shape[0]
    totals = state[6]
    ready = pl.ds(0, nx - HALO)
    stores = [
        pltpu.make_async_copy(state[3 + n].at[ready], out.at[ready], sems.at[n])
        for n, out in enumerate((lm_out, mm_out))
    ]
    for store in stores:
        store.start()
    fill_rim(state[0], nx + HALO, early, late)
    outer_pass((nx, nx - HALO), inv_ref, width_ref, state, scratch)
    for n in range(2):
        for c in range(totals.shape[1]):
            line = jnp.sum(totals[n, c], axis=0, keepdims=True)
            for member in range(copies.shape[0]):
                copies[member, n : n + 1, column(c)] = line
    for store in stores:
        store.wait()


def finish_kernel(
    planes, parts_ref, width_ref, lm_ref, mm_ref, size_ref, lm_in, mm_in,
    eddy_out, lm_out, mm_out, coefficient_ref,
    eddy_ref, sems,
):
    nx = lm_ref.shape[0]
    last = pl.ds(nx - HALO, HALO)
    stores = [
        pltpu.make_async_copy(ref.at[last], out.at[last], sems.at[n])
        for n, (ref, out) in enumerate(((lm_ref, lm_out), (mm_ref, mm_out)))
    ]
    for store in stores:
        store.start()
    total = parts_ref[0]
    for member in range(1, parts_ref.shape[0]):
        total = total + parts_ref[member]
    coefficient = total[0:1] / planes / (total[1:2] / planes + 1e-06)
    coefficient_ref[...] = coefficient[0]
    scale = (coefficient * width_ref[...])[None]
    for n in range(nx // HALO):
        part = pl.ds(HALO * n, HALO)
        eddy_ref[part] = scale * size_ref[part]
        stores.append(pltpu.make_async_copy(eddy_ref.at[part], eddy_out.at[part], sems.at[2 + n]))
        stores[-1].start()
    for store in stores:
        store.wait()


WHOLE = pl.BlockSpec(memory_space=pltpu.VMEM)
THERE = pl.BlockSpec(memory_space=pl.ANY)


def call(kernel, outs, scratch, flops, aliases, args, stored=()):
    return pl.pallas_call(
        kernel,
        out_shape=(
            *[pltpu.VMEM(shape, jnp.float32) for shape in outs],
            *[jax.ShapeDtypeStruct(shape, jnp.float32) for shape in stored],
        ),
        in_specs=[WHOLE] * len(args),
        out_specs=(*[WHOLE] * len(outs), *[THERE] * len(stored)),
        scratch_shapes=scratch,
        input_output_aliases=aliases,
        cost_estimate=pl.CostEstimate(flops=flops, bytes_accessed=0, transcendentals=0),
        compiler_params=pltpu.CompilerParams(vmem_limit_bytes=VMEM_LIMIT),
    )(*args)


VMEM_LIMIT = 16 * 2**20


def per_device(velocity, y_gap):
    _, nx, nz, ny = velocity.shape
    chunks, rows = ny // LANES, nz + 2 * SUB
    width_sq = width_square(y_gap)
    inverse = 2.0 / (y_gap[:-1] + y_gap[1:])
    lines = (inverse[None], width_sq[None])

    cells_shape = (3, nx + 2 * HALO, chunks, rows, LANES)
    field = (nx, nz, ny)
    early = (EARLY_DOWN, EARLY_UP)
    first_early, last_early, first_late, last_late, across, within, cells = call(
        split_kernel,
        [(3, HALO, e, ny) for e in early] + [(3, HALO, (nz - e) // QUAD, QUAD, ny) for e in early]
        + [(3, nx, HALO, ny)] * 2
        + [cells_shape],
        [], 0, {}, (velocity,),
    )
    across = send(across, GZ, lambda i: i + 1 if i % 2 else i - 1)
    within = send(within, GZ, lambda i: i - 1 if i % 2 else i + 1)
    before_early = send(last_early, GX, lambda i: i + 1)
    after_early = send(first_early, GX, lambda i: i - 1)
    first_late, last_late = call(
        join_kernel, [(3, HALO, nz // QUAD - e // QUAD + 1, QUAD, ny) for e in early],
        [], 0, {}, (across, within, first_late, last_late),
    )
    before_late = send(last_late, GX, lambda i: i + 1)
    after_late = send(first_late, GX, lambda i: i - 1)

    scratch = [
        pltpu.VMEM((chunks, rows, LANES), jnp.float32),
        pltpu.VMEM((12, chunks, rows, LANES), jnp.float32),
    ]
    state_shapes = [
        cells_shape,
        (12, nx + 2, chunks, nz, LANES),
        (3, nx + 2, chunks, rows, LANES),
        field, field, field,
        (2, chunks, SUB, LANES),
    ]
    state = call(
        inner_kernel, state_shapes, scratch, 20_000_000, {4: 0},
        (across, within, *lines, cells),
    )
    state = call(
        low_kernel, state_shapes, scratch, 10_000_000,
        {4 + n: n for n in range(STATE)}, (before_early, before_late, *lines, *state),
    )
    *state, copies, lm_out, mm_out = call(
        high_kernel, [*state_shapes, (members(GROUPS[0]), 2, ny)],
        [*scratch, pltpu.SemaphoreType.DMA((2,))], 10_000_000,
        {4 + n: n for n in range(STATE)}, (after_early, after_late, *lines, *state), [field] * 2,
    )
    lm_field, mm_field, strain_size = state[3:6]
    planes = nx * lax.axis_size(GX) * nz * lax.axis_size(GZ)
    block = jax.ShapeDtypeStruct(field, jnp.float32)
    eddy_visc, lm_field, mm_field, coefficient = pl.pallas_call(
        functools.partial(finish_kernel, planes),
        out_shape=(block, block, block, jax.ShapeDtypeStruct((ny,), jnp.float32)),
        in_specs=[WHOLE] * 5 + [THERE] * 2,
        out_specs=(THERE, THERE, THERE, WHOLE),
        scratch_shapes=[pltpu.VMEM(field, jnp.float32), pltpu.SemaphoreType.DMA((2 + nx // HALO,))],
        input_output_aliases={5: 1, 6: 2},
        name="finish",
        compiler_params=pltpu.CompilerParams(vmem_limit_bytes=VMEM_LIMIT),
    )(over_axes(copies), lines[1], lm_field, mm_field, strain_size, lm_out, mm_out)
    return (eddy_visc, lm_field, mm_field, coefficient)


def solution(mesh):
    torus = Mesh(mesh.devices.reshape(8, 2, 4, 2, 2), ("gx_0", "gx_1", "gz_0", "gz_1", "gz_2"))

    return jax.shard_map(
        per_device,
        mesh=torus,
        in_specs=(P(None, GX, GZ, None), P()),
        out_specs=(P(GX, GZ, None), P(GX, GZ, None), P(GX, GZ, None), P()),
        check_vma=False,
    )
```

```python
import functools

import jax
import jax.numpy as jnp
from jax import lax
from jax.experimental import pallas as pl
from jax.experimental.pallas import tpu as pltpu
from jax.sharding import Mesh
from jax.sharding import PartitionSpec as P


GX = ("gx_0", "gx_1")
GZ = ("gz_0", "gz_1", "gz_2")

LANES = 128
SUB = 8
TOP = 8
HALO = 2
EARLY_UP, EARLY_DOWN = 24, 24
QUAD = 2 * HALO


def send(array, axis, target):
    size = lax.axis_size(axis)
    return lax.ppermute(array, axis, [(i, target(i) % size) for i in range(size)])


def is_odd():
    return lax.axis_index("gz_2") == 1


def pick(odd, if_odd, if_even):
    return jnp.where(odd, if_odd, if_even)


GROUPS = (("gx_1", "gz_0", "gz_1", "gz_2"), ("gx_0",))


def members(axes):
    return functools.reduce(lambda count, axis: count * lax.axis_size(axis), axes, 1)


def over_axes(copies):
    half = jnp.sum(lax.all_to_all(copies, GROUPS[0], 0, 0, tiled=True), axis=0)
    copies = jnp.broadcast_to(half[None], (members(GROUPS[1]), *half.shape))
    return lax.all_to_all(copies, GROUPS[1], 0, 0, tiled=True)


def width_square(y_gap):
    return (0.5 * (y_gap[:-1] + y_gap[1:])) ** (2.0 / 3.0)


def strain_of(ref, slopes, at, chunk, row):
    def cell(k, step_x=0, step_z=0):
        return ref[k, at + step_x, chunk, pl.ds(row + step_z, SUB), :]

    along_x = [cell(k, 1) - cell(k, -1) for k in range(3)]
    along_z = [cell(k, 0, 1) - cell(k, 0, -1) for k in range(3)]
    parts = [
        along_x[0],
        slopes[1],
        along_z[2],
        slopes[0] + along_x[1],
        along_z[0] + along_x[2],
        along_z[1] + slopes[2],
    ]
    squares = [part * part for part in parts]
    square = 0.5 * (squares[0] + squares[1] + squares[2]) + 0.25 * (
        squares[3] + squares[4] + squares[5]
    )
    return parts, jnp.sqrt(square)


def wall_slopes(read, inverse, chunks):
    lane = lax.broadcasted_iota(jnp.int32, (SUB, LANES), 1)
    values = [read(c) for c in range(chunks)]
    ahead = [pltpu.roll(value, LANES - 1, 1) for value in values] + [jnp.zeros_like(values[0])]
    behind = [jnp.zeros_like(values[0])] + [pltpu.roll(value, 1, 1) for value in values]
    return [
        (
            jnp.where(lane == LANES - 1, ahead[c + 1], ahead[c])
            - jnp.where(lane == 0, behind[c], behind[c + 1])
        )
        * inverse[c]
        for c in range(chunks)
    ]


PAIRS = ((0, 0), (1, 1), (2, 2), (0, 1), (0, 2), (1, 2))


def smooth(below, here, above):
    return (below + above) + (here + here)


def column(c):
    return slice(c * LANES, (c + 1) * LANES)


def put_layer(cells, at, rows, value):
    for k in range(3):
        for c in range(value(k).shape[-1] // LANES):
            cells[k, at, c, rows, :] = value(k)[:, column(c)]


def split_kernel(v_ref, first_early, last_early, first_late, last_late, across, within):
    _, nx, nz, _ = v_ref.shape
    odd = is_odd()
    for k in range(3):
        for j in range(HALO):
            for at, head, tail in ((j, first_early, first_late), (nx - HALO + j, last_early, last_late)):
                early = head.shape[2]
                head[k, j] = v_ref[k, at, :early, :]
                for q in range(tail.shape[2]):
                    row = early + QUAD * q
                    tail[k, j, q] = v_ref[k, at, row : row + QUAD, :]
        for i in range(nx):
            first, last = v_ref[k, i, :HALO, :], v_ref[k, i, nz - HALO :, :]
            across[k, i] = pick(odd, last, first)
            within[k, i] = pick(odd, first, last)


def join_kernel(across, within, first_late, last_late, first_out, last_out):
    nx = across.shape[1]
    odd = is_odd()
    for k in range(3):
        for j in range(HALO):
            for at, late, out in ((j, first_late, first_out), (nx - HALO + j, last_late, last_out)):
                quads = late.shape[2]
                for q in range(quads):
                    out[k, j, q] = late[k, j, q]
                there, here = across[k, at], within[k, at]
                out[k, j, quads, :HALO, :] = pick(odd, here, there)
                out[k, j, quads, HALO:, :] = pick(odd, there, here)


def layer_pass(i, inverse, cells, filtered, smoothed, size_ref, sizes, products):
    chunks, nz = filtered.shape[2:4]
    nx = cells.shape[1] - 2 * HALO
    blocks = nz // SUB
    wide = [TOP - 1 + SUB * b for b in range(blocks + 1)]
    at = i + 1
    for row in wide:
        per_speed = [
            wall_slopes(lambda c: cells[k, at, c, pl.ds(row, SUB), :], inverse, chunks)
            for k in range(3)
        ]
        for c in range(chunks):
            parts, size = strain_of(cells, [per_speed[k][c] for k in range(3)], at, c, row)
            sizes[c, pl.ds(row, SUB), :] = size
            speeds = [cells[k, at, c, pl.ds(row, SUB), :] for k in range(3)]
            for n in range(6):
                products[n, c, pl.ds(row, SUB), :] = size * parts[n]
                p, q = PAIRS[n]
                products[6 + n, c, pl.ds(row, SUB), :] = speeds[p] * speeds[q]
    for c in range(chunks):
        for b in range(blocks):
            row = TOP + SUB * b
            for n in range(12):
                filtered[n, i, c, pl.ds(SUB * b, SUB), :] = smooth(
                    *[products[n, c, pl.ds(row + s, SUB), :] for s in (-1, 0, 1)]
                )

    @pl.when(jnp.logical_and(i >= 1, i <= nx))
    def _():
        for c in range(chunks):
            for b in range(blocks):
                size_ref[i - 1, SUB * b : SUB * (b + 1), column(c)] = sizes[
                    c, TOP + SUB * b : TOP + SUB * (b + 1), :
                ]

    for k in range(3):
        for c in range(chunks):
            for b in range(blocks + 2):
                row = SUB * b
                products[k, c, pl.ds(row, SUB), :] = smooth(
                    *[cells[k, at + s, c, pl.ds(row, SUB), :] for s in (-1, 0, 1)]
                )
            for row in wide:
                smoothed[k, i, c, pl.ds(row, SUB), :] = smooth(
                    *[products[k, c, pl.ds(row + s, SUB), :] for s in (-1, 0, 1)]
                )


def result_pass(i, inverse, width, filtered, smoothed, lm_ref, mm_ref, totals):
    chunks, nz = filtered.shape[2:4]
    at = i + 1
    add = functools.partial(functools.reduce, jnp.add)
    for b in range(nz // SUB):
        row = TOP + SUB * b
        per_speed = [
            wall_slopes(lambda c: smoothed[k, at, c, pl.ds(row, SUB), :], inverse, chunks)
            for k in range(3)
        ]
        for c in range(chunks):
            parts, size = strain_of(smoothed, [per_speed[k][c] for k in range(3)], at, c, row)
            size = 0.25 * size
            speeds = [0.25 * smoothed[k, at, c, pl.ds(row, SUB), :] for k in range(3)]

            def over_x(n):
                return smooth(*[filtered[n, i + s, c, pl.ds(SUB * b, SUB), :] for s in range(3)])

            cross, diagonal, outside = [], [], []
            for n in range(6):
                model = over_x(n) - size * parts[n]
                p, q = PAIRS[n]
                cross.append((over_x(6 + n) - speeds[p] * speeds[q]) * model)
                (diagonal if n < 3 else outside).append(model * model)
            lm = (width[c] * (1.0 / 256.0)) * add(cross)
            mm = (width[c] * width[c] * (1.0 / 256.0)) * (add(diagonal) + 0.5 * add(outside))
            lm_ref[i, SUB * b : SUB * (b + 1), column(c)] = lm
            mm_ref[i, SUB * b : SUB * (b + 1), column(c)] = mm
            totals[0, c] += lm
            totals[1, c] += mm


def rows_of(ref):
    return [
        jnp.broadcast_to(ref[:, column(c)], (SUB, LANES)) for c in range(ref.shape[-1] // LANES)
    ]


def inner_kernel(
    across, within, inv_ref, width_ref, v_ref,
    cells, filtered, smoothed, lm_ref, mm_ref, size_ref, totals,
    sizes, products,
):
    nx, nz, _ = lm_ref.shape

    odd = is_odd()

    def sides(i, carry):
        put_layer(cells, i + HALO, slice(TOP, TOP + nz), lambda k: v_ref[k, i])
        for rows, flip in ((slice(TOP - HALO, TOP), False), (slice(TOP + nz, TOP + nz + HALO), True)):
            there, here = (across, within) if flip else (within, across)
            put_layer(cells, i + HALO, rows, lambda k: pick(odd, there[k, i], here[k, i]))
        return carry

    lax.fori_loop(0, nx, sides, 0)
    inverse, width = rows_of(inv_ref), rows_of(width_ref)

    def layer(i, carry):
        layer_pass(i, inverse, cells, filtered, smoothed, size_ref, sizes, products)
        return carry

    lax.fori_loop(HALO, nx, layer, 0)
    totals[...] = jnp.zeros_like(totals)

    def result(i, carry):
        result_pass(i, inverse, width, filtered, smoothed, lm_ref, mm_ref, totals)
        return carry

    lax.fori_loop(HALO, nx - HALO, result, 0)


STATE = 7


def outer_pass(layers, inv_ref, width_ref, state, scratch):
    cells, filtered, smoothed, lm_ref, mm_ref, size_ref, totals = state
    inverse, width = rows_of(inv_ref), rows_of(width_ref)

    def layer(j, carry):
        layer_pass(layers[0] + j, inverse, cells, filtered, smoothed, size_ref, *scratch)
        return carry

    lax.fori_loop(0, HALO, layer, 0, unroll=True)

    def result(j, carry):
        result_pass(layers[1] + j, inverse, width, filtered, smoothed, lm_ref, mm_ref, totals)
        return carry

    lax.fori_loop(0, HALO, result, 0, unroll=True)


def fill_rim(cells, at, early, late):
    head, quads = early.shape[2], late.shape[2] - 1
    end = TOP + head + QUAD * quads
    for j in range(HALO):
        put_layer(cells, at + j, slice(TOP, TOP + head), lambda k: early[k, j])
        for q in range(quads):
            row = TOP + head + QUAD * q
            put_layer(cells, at + j, slice(row, row + QUAD), lambda k: late[k, j, q])
        put_layer(cells, at + j, slice(TOP - HALO, TOP), lambda k: late[k, j, quads, :HALO, :])
        put_layer(cells, at + j, slice(end, end + HALO), lambda k: late[k, j, quads, HALO:, :])


def low_kernel(early, late, inv_ref, width_ref, *refs):
    state, scratch = refs[STATE : 2 * STATE], refs[2 * STATE :]
    fill_rim(state[0], 0, early, late)
    outer_pass((0, 0), inv_ref, width_ref, state, scratch)


def high_kernel(early, late, inv_ref, width_ref, *refs):
    state, (copies, lm_out, mm_out, *scratch, sems) = refs[STATE : 2 * STATE], refs[2 * STATE :]
    nx = state[3].shape[0]
    totals = state[6]
    ready = pl.ds(0, nx - HALO)
    stores = [
        pltpu.make_async_copy(state[3 + n].at[ready], out.at[ready], sems.at[n])
        for n, out in enumerate((lm_out, mm_out))
    ]
    for store in stores:
        store.start()
    fill_rim(state[0], nx + HALO, early, late)
    outer_pass((nx, nx - HALO), inv_ref, width_ref, state, scratch)
    for n in range(2):
        for c in range(totals.shape[1]):
            line = jnp.sum(totals[n, c], axis=0, keepdims=True)
            for member in range(copies.shape[0]):
                copies[member, n : n + 1, column(c)] = line
    for store in stores:
        store.wait()


def finish_kernel(
    planes, parts_ref, width_ref, lm_ref, mm_ref, size_ref, lm_in, mm_in,
    eddy_out, lm_out, mm_out, coefficient_ref,
    eddy_ref, sems,
):
    nx = lm_ref.shape[0]
    last = pl.ds(nx - HALO, HALO)
    stores = [
        pltpu.make_async_copy(ref.at[last], out.at[last], sems.at[n])
        for n, (ref, out) in enumerate(((lm_ref, lm_out), (mm_ref, mm_out)))
    ]
    for store in stores:
        store.start()
    total = parts_ref[0]
    for member in range(1, parts_ref.shape[0]):
        total = total + parts_ref[member]
    coefficient = total[0:1] / planes / (total[1:2] / planes + 1e-06)
    coefficient_ref[...] = coefficient[0]
    scale = (coefficient * width_ref[...])[None]
    for n in range(nx // HALO):
        part = pl.ds(HALO * n, HALO)
        eddy_ref[part] = scale * size_ref[part]
        stores.append(pltpu.make_async_copy(eddy_ref.at[part], eddy_out.at[part], sems.at[2 + n]))
        stores[-1].start()
    for store in stores:
        store.wait()


WHOLE = pl.BlockSpec(memory_space=pltpu.VMEM)
THERE = pl.BlockSpec(memory_space=pl.ANY)


def call(kernel, outs, scratch, flops, aliases, args, stored=()):
    return pl.pallas_call(
        kernel,
        out_shape=(
            *[pltpu.VMEM(shape, jnp.float32) for shape in outs],
            *[jax.ShapeDtypeStruct(shape, jnp.float32) for shape in stored],
        ),
        in_specs=[WHOLE] * len(args),
        out_specs=(*[WHOLE] * len(outs), *[THERE] * len(stored)),
        scratch_shapes=scratch,
        input_output_aliases=aliases,
        cost_estimate=pl.CostEstimate(flops=flops, bytes_accessed=0, transcendentals=0),
        compiler_params=pltpu.CompilerParams(vmem_limit_bytes=VMEM_LIMIT),
    )(*args)


VMEM_LIMIT = 16 * 2**20


def per_device(velocity, y_gap):
    _, nx, nz, ny = velocity.shape
    chunks, rows = ny // LANES, nz + 2 * SUB
    width_sq = width_square(y_gap)
    inverse = 2.0 / (y_gap[:-1] + y_gap[1:])
    lines = (inverse[None], width_sq[None])

    cells_shape = (3, nx + 2 * HALO, chunks, rows, LANES)
    field = (nx, nz, ny)
    early = (EARLY_DOWN, EARLY_UP)
    first_early, last_early, first_late, last_late, across, within = call(
        split_kernel,
        [(3, HALO, e, ny) for e in early] + [(3, HALO, (nz - e) // QUAD, QUAD, ny) for e in early]
        + [(3, nx, HALO, ny)] * 2,
        [], 0, {}, (velocity,),
    )
    across = send(across, GZ, lambda i: i + 1 if i % 2 else i - 1)
    within = send(within, GZ, lambda i: i - 1 if i % 2 else i + 1)
    before_early = send(last_early, GX, lambda i: i + 1)
    after_early = send(first_early, GX, lambda i: i - 1)
    first_late, last_late = call(
        join_kernel, [(3, HALO, nz // QUAD - e // QUAD + 1, QUAD, ny) for e in early],
        [], 0, {}, (across, within, first_late, last_late),
    )
    before_late = send(last_late, GX, lambda i: i + 1)
    after_late = send(first_late, GX, lambda i: i - 1)

    scratch = [
        pltpu.VMEM((chunks, rows, LANES), jnp.float32),
        pltpu.VMEM((12, chunks, rows, LANES), jnp.float32),
    ]
    state_shapes = [
        cells_shape,
        (12, nx + 2, chunks, nz, LANES),
        (3, nx + 2, chunks, rows, LANES),
        field, field, field,
        (2, chunks, SUB, LANES),
    ]
    state = call(
        inner_kernel, state_shapes, scratch, 20_000_000, {},
        (across, within, *lines, velocity),
    )
    state = call(
        low_kernel, state_shapes, scratch, 10_000_000,
        {4 + n: n for n in range(STATE)}, (before_early, before_late, *lines, *state),
    )
    *state, copies, lm_out, mm_out = call(
        high_kernel, [*state_shapes, (members(GROUPS[0]), 2, ny)],
        [*scratch, pltpu.SemaphoreType.DMA((2,))], 10_000_000,
        {4 + n: n for n in range(STATE)}, (after_early, after_late, *lines, *state), [field] * 2,
    )
    lm_field, mm_field, strain_size = state[3:6]
    planes = nx * lax.axis_size(GX) * nz * lax.axis_size(GZ)
    block = jax.ShapeDtypeStruct(field, jnp.float32)
    eddy_visc, lm_field, mm_field, coefficient = pl.pallas_call(
        functools.partial(finish_kernel, planes),
        out_shape=(block, block, block, jax.ShapeDtypeStruct((ny,), jnp.float32)),
        in_specs=[WHOLE] * 5 + [THERE] * 2,
        out_specs=(THERE, THERE, THERE, WHOLE),
        scratch_shapes=[pltpu.VMEM(field, jnp.float32), pltpu.SemaphoreType.DMA((2 + nx // HALO,))],
        input_output_aliases={5: 1, 6: 2},
        name="finish",
        compiler_params=pltpu.CompilerParams(vmem_limit_bytes=VMEM_LIMIT),
    )(over_axes(copies), lines[1], lm_field, mm_field, strain_size, lm_out, mm_out)
    return (eddy_visc, lm_field, mm_field, coefficient)


def solution(mesh):
    torus = Mesh(mesh.devices.reshape(8, 2, 4, 2, 2), ("gx_0", "gx_1", "gz_0", "gz_1", "gz_2"))

    return jax.shard_map(
        per_device,
        mesh=torus,
        in_specs=(P(None, GX, GZ, None), P()),
        out_specs=(P(GX, GZ, None), P(GX, GZ, None), P(GX, GZ, None), P()),
        check_vma=False,
    )
```
